128 devices in a mesh: gy: 16 (over z, x), gz: 8 (over y, core).
Axes of the slice: x: 4, y: 4, z: 4, core: 2. Of those that a mesh axis runs over, the one named last changes fastest.
Arguments:
- fraction: float32 [128, 128, 1024], P('gz', 'gy'), may hold values from 0 to 1
- velocity_x: float32 [128, 128, 1024], P('gz', 'gy'), may hold values from -9 to 9
- velocity_y: float32 [128, 128, 1024], P('gz', 'gy'), may hold values from -9 to 9
- velocity_z: float32 [128, 128, 1024], P('gz', 'gy'), may hold values from -9 to 9
Outputs:
- advected: float32 [128, 128, 1024], P('gz', 'gy')
- time_step: float32 [], replicated
The draws below stay inside these ranges and needn't reach their ends.
All inputs are finite; a program needn't handle non-finite values. Where the reference program divides by a largest or mean magnitude, that divisor is 1e-20 or more.
Results may differ from the reference program's by a relative error of at most 0.0003.
Values sent between devices are 32-bit elements; how exact they have to be, the bound alone decides.
A program may use at most 64 MiB of HBM per device.

```python
import jax
import jax.numpy as jnp

NX = 1024
CY = 8
CZ = 16
NEWTON = 5
NY = 128
NZ = 128
N_GY = 16
N_GZ = 8


def block_linear():
    plane_owner = jnp.arange(NZ) // CZ
    row_owner = jnp.arange(NY) // CY
    return row_owner[None, :] * N_GZ + plane_owner[:, None]


def spread_blocks(values):
    return values[block_linear()][:, :, None]


def draw_fraction(key, part):
    key_pick, key_coin, key_value, key_level, key_jitter, key_power = jax.random.split(key, 6)
    count = N_GY * N_GZ
    linear = jnp.arange(count).astype(jnp.float32)
    rise = 0.5 + linear / (count - 1)
    level = jax.random.uniform(key_level, (), jnp.float32, 0.15, 0.45)
    jitter = jnp.exp(jax.random.uniform(key_jitter, (count,), jnp.float32, jnp.log(0.6), jnp.log(1.4)))
    mixed_rate = spread_blocks(level * rise * jitter)
    power = jax.random.uniform(key_power, (count,), jnp.float32, 1.0, 2.0)
    chooser = jax.random.uniform(key_pick, (NZ, NY, NX), jnp.float32)
    pure_value = (jax.random.uniform(key_coin, (NZ, NY, NX), jnp.float32) < 0.5).astype(jnp.float32)
    mixture = jax.random.uniform(key_value, (NZ, NY, NX), jnp.float32)
    mixture = jnp.power(mixture, spread_blocks(power))
    return jnp.where(chooser < mixed_rate, mixture, pure_value)


def speed_field(key, which):
    local_key = jax.random.fold_in(key, which)
    key_values, key_peak, key_lower, key_upper = jax.random.split(local_key, 4)
    count = N_GY * N_GZ
    half = count // 2
    ranks = jnp.concatenate([jax.random.permutation(key_lower, half), half + jax.random.permutation(key_upper, count - half)]).astype(jnp.float32)
    peak = jax.random.uniform(key_peak, (), jnp.float32, 3.0, 9.0)
    amplitude = peak * (1.0 + 2.0 * ranks / (count - 1)) / 3.0
    values = jnp.clip(jax.random.normal(key_values, (NZ, NY, NX), jnp.float32), -3.0, 3.0) / 3.0
    return values * spread_blocks(amplitude)


def draw_velocity_x(key, part):
    return speed_field(key, 11)


def draw_velocity_y(key, part):
    return speed_field(key, 23)


def draw_velocity_z(key, part):
    return speed_field(key, 37)


def setup_inputs(seed: int = 0) -> dict:
    key_of = jax.random.split(jax.random.key(seed), 5)
    fraction = draw_fraction(jax.random.fold_in(key_of[4], 71), 0)
    velocity_x = draw_velocity_x(jax.random.fold_in(key_of[4], 71), 0)
    velocity_y = draw_velocity_y(jax.random.fold_in(key_of[4], 71), 0)
    velocity_z = draw_velocity_z(jax.random.fold_in(key_of[4], 71), 0)
    return dict(fraction=fraction, velocity_x=velocity_x, velocity_y=velocity_y, velocity_z=velocity_z)


tilt_floor = 0.1
courant = 0.45
epsilon = 1e-6


def cube_step(reach, height):
    safe = jnp.where(height > 0, height, 1.0)
    whole = 3.0 * reach * reach - 3.0 * reach * height + height * height
    partial_part = reach * reach * reach / safe
    return jnp.where(reach - height >= 0, whole, jnp.where(reach >= 0, partial_part, 0.0))


def cube_rate(reach, height):
    safe = jnp.where(height > 0, height, 1.0)
    whole = 6.0 * reach - 3.0 * height
    partial_part = 3.0 * reach * reach / safe
    return jnp.where(reach - height >= 0, whole, jnp.where(reach >= 0, partial_part, 0.0))


def region_volume(offset, tilt_a, tilt_b, height, extent):
    combo = cube_step(offset, height) - cube_step(offset - tilt_a, height) - cube_step(offset - tilt_b, height) + cube_step(offset - tilt_a - tilt_b, height)
    return extent * combo / (6.0 * tilt_a * tilt_b)


def section_area(offset, tilt_a, tilt_b, height):
    combo = cube_rate(offset, height) - cube_rate(offset - tilt_a, height) - cube_rate(offset - tilt_b, height) + cube_rate(offset - tilt_a - tilt_b, height)
    return combo / (6.0 * tilt_a * tilt_b)


def youngs_slope(padded):
    def smooth_zero(arr):
        return arr[:-2] + 2.0 * arr[1:-1] + arr[2:]

    def smooth_one(arr):
        return arr[:, :-2] + 2.0 * arr[:, 1:-1] + arr[:, 2:]

    def smooth_cells(arr):
        return jnp.roll(arr, 1, 2) + 2.0 * arr + jnp.roll(arr, -1, 2)

    diff_zero = padded[2:] - padded[:-2]
    diff_one = padded[:, 2:] - padded[:, :-2]
    diff_cells = jnp.roll(padded, -1, 2) - jnp.roll(padded, 1, 2)
    grad_zero = smooth_cells(smooth_one(diff_zero)) / 32.0
    grad_one = smooth_cells(smooth_zero(diff_one)) / 32.0
    grad_cells = smooth_one(smooth_zero(diff_cells)) / 32.0
    return (grad_zero, grad_one, grad_cells)


def plane_for(fraction, slopes, axis_dim):
    slope_d = slopes[axis_dim]
    across = [slopes[index] for index in range(3) if index != axis_dim]
    tilt_d = jnp.abs(slope_d)
    tilt_a = jnp.abs(across[0]) + tilt_floor
    tilt_b = jnp.abs(across[1]) + tilt_floor
    volume = jnp.clip(fraction, 0.0, 1.0)
    lesser = jnp.minimum(volume, 1.0 - volume)
    summed = tilt_a + tilt_b + tilt_d
    offset = 0.5 * summed
    for repeat in range(NEWTON):
        offset = offset - (region_volume(offset, tilt_a, tilt_b, tilt_d, 1.0) - lesser) / section_area(offset, tilt_a, tilt_b, tilt_d)
    offset = jnp.where(volume > 0.5, summed - offset, offset)
    return (offset, tilt_a, tilt_b, tilt_d, slope_d > 0)


def outflow(planes, width, upward):
    offset, tilt_a, tilt_b, tilt_d, mirrored = planes
    if upward:
        start_at = jnp.where(mirrored, 0.0, 1.0 - width)
    else:
        start_at = jnp.where(mirrored, 1.0 - width, 0.0)
    return region_volume(offset - tilt_d * start_at, tilt_a, tilt_b, tilt_d * width, width)


def sweep(fraction, velocity, axis_dim, time_step):
    padded = jnp.pad(fraction, ((1, 1), (1, 1), (0, 0)), mode="wrap")
    planes = plane_for(fraction, youngs_slope(padded), axis_dim)
    velocity_low = jnp.roll(velocity, 1, axis_dim)
    out_upper = outflow(planes, jnp.maximum(time_step * velocity, 0.0), True)
    out_lower = outflow(planes, jnp.maximum(-time_step * velocity_low, 0.0), False)
    from_below = jnp.roll(out_upper, 1, axis_dim)
    from_above = jnp.roll(out_lower, -1, axis_dim)
    divisor = 1.0 - time_step * velocity + time_step * velocity_low
    return (fraction - out_upper - out_lower + from_below + from_above) / divisor


def reference(fraction, velocity_x, velocity_y, velocity_z):
    umax = jnp.maximum(jnp.maximum(jnp.max(jnp.abs(velocity_x)), jnp.max(jnp.abs(velocity_y))), jnp.max(jnp.abs(velocity_z)))
    share = jnp.sum(4.0 * fraction * (1.0 - fraction)) / (NX * NY * NZ)
    time_step = courant / ((umax + epsilon) * (1.0 + share))
    field = sweep(fraction, velocity_x, 2, time_step)
    field = sweep(field, velocity_y, 1, time_step)
    field = sweep(field, velocity_z, 0, time_step)
    return field, time_step
```

```python
import functools

import jax
import jax.numpy as jnp
from jax import lax
from jax.experimental import pallas as pl
from jax.experimental.pallas import tpu as pltpu
from jax.sharding import PartitionSpec as P

NEWTON = 5
LANES = 128
GROUP = 8

tilt_floor = 0.1
courant = 0.45
epsilon = 1e-06
tiny = 1e-30

MESH = pl.DeviceIdType.MESH


def lane_of(value):
    return lax.broadcasted_iota(jnp.int32, value.shape, value.ndim - 1)


def x_next(value):
    turned = pltpu.roll(value, LANES - 1, value.ndim - 1)
    carried = pltpu.roll(turned, value.shape[-2] - 1, value.ndim - 2)
    return jnp.where(lane_of(value) == LANES - 1, carried, turned)


def x_prev(value):
    turned = pltpu.roll(value, 1, value.ndim - 1)
    carried = pltpu.roll(turned, 1, value.ndim - 2)
    return jnp.where(lane_of(value) == 0, carried, turned)


def solve_offset(g, tilt_a, tilt_b, tilt_d):
    volume = jnp.clip(g, 0.0, 1.0)
    lesser = jnp.minimum(volume, 1.0 - volume)
    low = jnp.minimum(tilt_a, tilt_b)
    high = jnp.maximum(tilt_a, tilt_b)
    n1 = jnp.minimum(low, tilt_d)
    middle = jnp.maximum(low, tilt_d)
    n2 = jnp.minimum(middle, high)
    n3 = jnp.maximum(middle, high)
    summed = tilt_a + tilt_b + tilt_d
    inverse = 1.0 / jnp.maximum(n1, tiny)
    third = inverse * (1.0 / 3.0)
    product = n2 * n3
    target = 2.0 * product * lesser
    gap = jnp.maximum(n1 + n2 - n3, 0.0)
    rate = 2.0 * n2 - 0.5 * gap * (gap * inverse)
    offset = 0.5 * summed - (product - target) / rate
    for repeat in range(NEWTON - 1):
        p1 = jnp.minimum(offset, n1)
        q1 = offset - p1
        m2 = jnp.maximum(offset - n2, 0.0)
        p2 = jnp.minimum(m2, n1)
        q2 = m2 - p2
        p3 = jnp.minimum(jnp.maximum(offset - n3, 0.0), n1)
        s1, s2, s3 = p1 * p1, p2 * p2, p3 * p3
        squares = s1 - s2 - s3
        cubes = s1 * p1 - s2 * p2 - s3 * p3
        q = q1 - q2
        rate = squares * inverse + (q + q)
        volume_part = cubes * third + q * (q1 + q2 + n1)
        offset = offset - (volume_part - target) / rate
    return jnp.where(volume > 0.5, summed - offset, offset)


def face_flux(cross, offset, tilt_a, tilt_b, slope):
    turn = slope * cross
    height = jnp.abs(turn)
    reach = offset - jnp.where(turn > 0, 0.0, jnp.abs(slope) - height)

    def parts(value):
        inside = jnp.maximum(value, 0.0)
        p = jnp.minimum(inside, height)
        q = inside - p
        return p * p * p, q * (q + height)

    reach_a = reach - tilt_a
    p0, q0 = parts(reach)
    p1, q1 = parts(reach_a)
    p2, q2 = parts(reach - tilt_b)
    p3, q3 = parts(reach_a - tilt_b)
    cubes = (p0 - p1) - (p2 - p3)
    wholes = (q0 - q1) - (q2 - q3)
    combo = cubes * ((1.0 / 3.0) / jnp.maximum(height, tiny)) + wholes
    return cross * combo / (2.0 * tilt_a * tilt_b)


def kernel(
    n_gy, n_gz, f_hbm, vx_hbm, vy_hbm, vz_hbm, out_ref, dt_ref,
    f_ref, vx_ref, vy_ref, vz_ref, load_sem,
    g0, g1, g2, sx0, dx0, sx1, dx1, sx2, dx2,
    off0, ta0, tb0, sd0, off1, ta1, tb1, sd1, off2, ta2, tb2, sd2,
    vx, vy, vz, fy, fz, part_y, part_z,
    halo0_send, halo0_recv, halo1_send, halo1_recv, halo2_send, halo2_recv,
    vel_send, vel_recv, py_send, py_recv, pz_send, pz_recv,
):
    Z = f_ref.shape[0]
    T = sx0.shape[2]
    Y = f_ref.shape[1] // T
    loads = []
    for i, (source, target) in enumerate(
        ((f_hbm, f_ref), (vx_hbm, vx_ref), (vy_hbm, vy_ref), (vz_hbm, vz_ref))
    ):
        loads.append(pltpu.make_async_copy(source, target, load_sem.at[i]))
        loads[-1].start()
    my = lax.axis_index("gy")
    mz = lax.axis_index("gz")

    def at(dz, dy):
        return {
            "gy": lax.rem(my + dy + n_gy, n_gy),
            "gz": lax.rem(mz + dz + n_gz, n_gz),
        }

    barrier = pltpu.get_barrier_semaphore()
    greeted = [(0, i) for i in range(1, n_gy)] + [(i, 0) for i in range(1, n_gz)]
    greeted += [(a, b) for a in (-1, 1) for b in (-1, 1)]
    for dz, dy in greeted:
        pl.semaphore_signal(barrier, inc=1, device_id=at(dz, dy), device_id_type=MESH)

    def rows_of(ref, z, y):
        return ref[z, pl.ds(y, T, stride=Y), :]

    def gather(low, high, body, carry):
        count = high - low
        grouped = max(u for u in range(1, GROUP + 1) if count % u == 0)

        def step(i, carry):
            for u in range(grouped):
                carry = body(low + i * grouped + u, carry)
            return carry
        return lax.fori_loop(0, count // grouped, step, carry)

    def loop(low, high, body):
        def step(i, carry):
            body(i)
            return carry
        gather(low, high, step, 0)

    def halo_copies(g, spans, sends, recvs):
        copies = []
        for index, (dz, dy, src_z, dst_z, src_y, dst_y) in enumerate(spans):
            copies.append(pltpu.make_async_remote_copy(
                src_ref=g.at[src_z, src_y],
                dst_ref=g.at[dst_z, dst_y],
                send_sem=sends.at[index],
                recv_sem=recvs.at[index],
                device_id=at(dz, dy),
                device_id_type=MESH,
            ))
        return copies

    def span(side, count, pad, depth):
        if side == 0:
            return pl.ds(pad, count), pl.ds(pad, count)
        if side > 0:
            return pl.ds(pad + count - depth, depth), pl.ds(pad - depth, depth)
        return pl.ds(pad, depth), pl.ds(pad + count, depth)

    def spans_for(sides, pad_z, pad_y):
        return [
            (dz, dy, *span(dz, Z, pad_z, pad_z), *span(dy, Y, pad_y, pad_y))
            for dz, dy in sides
        ]

    Y_SIDES = [(0, -1), (0, 1)]
    Z_SIDES = [(a, b) for a in (-1, 1) for b in (0, -1, 1)]

    def fill(z, total):
        for y in range(Y):
            f = rows_of(f_ref, z, y)
            g0[z + 1, y + 1] = f
            total = total + 4.0 * f * (1.0 - f)
        return total

    loads[0].wait()
    total = gather(0, Z, fill, jnp.zeros((T, LANES), jnp.float32))

    def fill_velocity(z, peak):
        for y in range(Y):
            a = rows_of(vx_ref, z, y)
            b = rows_of(vy_ref, z, y)
            c = rows_of(vz_ref, z, y)
            vx[z, y] = a
            vy[z, y + 1] = b
            vz[z + 1, y] = c
            peak = jnp.maximum(peak, jnp.maximum(jnp.abs(a), jnp.maximum(jnp.abs(b), jnp.abs(c))))
        return peak

    for copy in loads[1:]:
        copy.wait()
    peak = gather(0, Z, fill_velocity, jnp.zeros((T, LANES), jnp.float32))
    first_row = lax.broadcasted_iota(jnp.int32, (T, LANES), 0) == 0

    def joined(sums, peaks):
        sums = jnp.broadcast_to(jnp.sum(sums, axis=0, keepdims=True), (T, LANES))
        peaks = jnp.broadcast_to(jnp.max(peaks, axis=0, keepdims=True), (T, LANES))
        return jnp.where(first_row, sums, peaks)

    def gathered(part, count):
        sums = part[0]
        peaks = part[0]
        for i in range(1, count):
            sums = sums + part[i]
            peaks = jnp.maximum(peaks, part[i])
        return jnp.where(first_row, sums, 0.0), jnp.where(first_row, 0.0, peaks)

    part_y[my] = joined(total, peak)
    pl.semaphore_wait(barrier, len(greeted))
    vel_copies = [
        pltpu.make_async_remote_copy(
            src_ref=vy.at[:, pl.ds(Y, 1)], dst_ref=vy.at[:, pl.ds(0, 1)],
            send_sem=vel_send.at[0], recv_sem=vel_recv.at[0],
            device_id=at(0, 1), device_id_type=MESH,
        ),
        pltpu.make_async_remote_copy(
            src_ref=vz.at[pl.ds(Z, 1)], dst_ref=vz.at[pl.ds(0, 1)],
            send_sem=vel_send.at[1], recv_sem=vel_recv.at[1],
            device_id=at(1, 0), device_id_type=MESH,
        ),
    ]

    def part_copies(part, mine, send, recv, count, along_y):
        copies = []
        for i in range(1, count):
            copies.append(pltpu.make_async_remote_copy(
                src_ref=part.at[mine], dst_ref=part.at[mine],
                send_sem=send.at[i - 1], recv_sem=recv.at[i - 1],
                device_id=at(0, i) if along_y else at(i, 0), device_id_type=MESH,
            ))
        return copies

    y_parts = part_copies(part_y, my, py_send, py_recv, n_gy, True)
    for copy in y_parts:
        copy.start()
    halos0 = halo_copies(g0, spans_for(Y_SIDES + Z_SIDES, 1, 1), halo0_send, halo0_recv)
    for copy in halos0:
        copy.start()
    for copy in vel_copies:
        copy.start()

    def smooth_rows(g, sx, dx, z, y, kz, ky):
        value = g[pl.ds(z, kz), pl.ds(y, ky)]
        pair = value + x_next(value)
        pair_before = x_prev(pair)
        sx[pl.ds(z, kz), pl.ds(y, ky)] = pair + pair_before
        dx[pl.ds(z, kz), pl.ds(y, ky)] = pair - pair_before

    def smooth_zero(arr):
        mid = arr[1:-1]
        return (arr[:-2] + mid) + (mid + arr[2:])

    def smooth_one(arr):
        pair = arr[:, :-1] + arr[:, 1:]
        return pair[:, :-1] + pair[:, 1:]

    def plane(refs, dim, z, y, kz, ky, parts=1):
        g, sx, dx, off, ta, tb, sd = refs
        s = sx[pl.ds(z, kz + 2), pl.ds(y, ky + 2)]
        d = dx[pl.ds(z, kz + 2), pl.ds(y, ky + 2)]
        grad_zero = smooth_one(s[2:] - s[:-2]) * (1.0 / 32.0)
        across = smooth_zero(s)
        grad_one = (across[:, 2:] - across[:, :-2]) * (1.0 / 32.0)
        grad_cells = smooth_one(smooth_zero(d)) * (1.0 / 32.0)
        slopes = (grad_zero, grad_one, grad_cells)
        low = 0
        for part in range(parts):
            count = (ky - low) // (parts - part)
            cut = [value[:, low:low + count] for value in slopes]
            slope = cut[dim]
            tilt_a, tilt_b = [jnp.abs(cut[e]) + tilt_floor for e in range(3) if e != dim]
            value = g[pl.ds(z + 1, kz), pl.ds(y + 1 + low, count)]
            where = (pl.ds(z, kz), pl.ds(y + low, count))
            off[where] = solve_offset(value, tilt_a, tilt_b, jnp.abs(slope))
            ta[where] = tilt_a
            tb[where] = tilt_b
            sd[where] = slope
            low += count

    def block(body, zs, y, ky, kz=1):
        count = len(zs) // kz
        step = zs[1] - zs[0] if len(zs) > 1 else 1
        loop(0, count, lambda i: body(zs[0] + step * kz * i, y, kz, ky))

    def planes(refs, dim, parts=1):
        return lambda z, y, kz, ky: plane(refs, dim, z, y, kz, ky, parts)

    def smooths(refs):
        return lambda z, y, kz, ky: smooth_rows(refs[0], refs[1], refs[2], z, y, kz, ky)

    own = range(0, Z)
    refs0 = (g0, sx0, dx0, off0, ta0, tb0, sd0)
    refs1 = (g1, sx1, dx1, off1, ta1, tb1, sd1)
    refs2 = (g2, sx2, dx2, off2, ta2, tb2, sd2)

    half = Z // 2
    block(smooths(refs0), range(1, Z + 1), 1, Y)
    block(planes(refs0, 2, 2), range(1, half), 1, Y - 2)
    for copy in y_parts:
        copy.wait()
    part_z[mz] = joined(*gathered(part_y, n_gy))
    z_parts = part_copies(part_z, mz, pz_send, pz_recv, n_gz, False)
    for copy in z_parts:
        copy.start()
    block(planes(refs0, 2, 2), range(half, Z - 1), 1, Y - 2)
    for copy in halos0:
        copy.wait()
    block(smooths(refs0), (0, Z + 1), 0, Y + 2)
    block(smooths(refs0), range(1, Z + 1), 0, 1)
    block(smooths(refs0), range(1, Z + 1), Y + 1, 1)
    block(planes(refs0, 2), own, 0, 1, 2)
    block(planes(refs0, 2), own, Y - 1, 1, 2)
    block(planes(refs0, 2, 2), (0, Z - 1), 1, Y - 2)

    def donors(z, y, kz, ky):
        where = (pl.ds(z, kz), pl.ds(y, ky))
        upward = vx[where] > 0
        for ref in (off0, ta0, tb0, sd0):
            value = ref[where]
            ref[where] = jnp.where(upward, value, x_next(value))

    block(donors, own, 0, Y // 2)
    block(donors, own, Y // 2, Y - Y // 2)
    for copy in z_parts:
        copy.wait()
    sums, peaks = gathered(part_z, n_gz)
    cells_all = float(Z * Y * T * LANES * n_gy * n_gz)
    share = jnp.broadcast_to(jnp.sum(sums, keepdims=True), (T, LANES)) / cells_all
    umax = jnp.broadcast_to(jnp.max(peaks, keepdims=True), (T, LANES))
    step_value = courant / ((umax + epsilon) * (1.0 + share))
    dt_ref[0, 0] = jnp.max(step_value)
    dt = step_value[None, None]

    def x_update(z, y, kz, ky):
        where = (pl.ds(z, kz), pl.ds(y, ky))
        cross = dt * vx[where]
        flux = face_flux(cross, off0[where], ta0[where], tb0[where], sd0[where])
        value = g0[pl.ds(z + 1, kz), pl.ds(y + 1, ky)]
        g1[pl.ds(z + 1, kz), pl.ds(y + 2, ky)] = (value - flux + x_prev(flux)) / (
            1.0 - cross + x_prev(cross)
        )

    deep = spans_for([(a, b) for a in (-1, 1) for b in (-1, 1)], 1, 2)
    spans1 = []
    for depth in (1, 2):
        for dy in (-1, 1):
            src, dst = span(dy, Y, 2, 2)
            near = (0, 1)[(dy > 0) == (depth == 1)]
            spans1.append((
                0, dy, pl.ds(1, Z), pl.ds(1, Z),
                pl.ds(src.start + near, 1), pl.ds(dst.start + near, 1),
            ))
    for dz in (-1, 1):
        spans1.append((dz, 0, *span(dz, Z, 1, 1), pl.ds(2, Y), pl.ds(2, Y)))
    spans1 += deep
    halos1 = halo_copies(g1, spans1, halo1_send, halo1_recv)

    block(x_update, own, 0, 1, 2)
    block(x_update, own, Y - 1, 1, 2)
    for copy in halos1[:2]:
        copy.start()
    block(x_update, own, 1, 1, 2)
    block(x_update, own, Y - 2, 1, 2)
    for copy in halos1[2:4]:
        copy.start()
    block(x_update, (0, Z - 1), 2, Y - 4)
    for copy in halos1[4:]:
        copy.start()
    block(x_update, range(1, Z - 1), 2, Y - 4)
    for copy in vel_copies:
        copy.wait()

    block(smooths(refs1), range(1, Z + 1), 2, Y)
    block(planes(refs1, 1, 2), range(1, Z - 1), 2, Y - 2)
    for copy in halos1[:2]:
        copy.wait()
    block(smooths(refs1), range(1, Z + 1), 1, 1)
    block(smooths(refs1), range(1, Z + 1), Y + 2, 1)
    block(planes(refs1, 1), range(1, Z - 1), 1, 1, 2)
    block(planes(refs1, 1), range(1, Z - 1), Y, 1, 2)
    for copy in halos1[2:]:
        copy.wait()
    block(smooths(refs1), (0, Z + 1), 0, Y + 4)
    block(smooths(refs1), range(1, Z + 1), 0, 1)
    block(smooths(refs1), range(1, Z + 1), Y + 3, 1)
    block(planes(refs1, 1, 3), (0, Z - 1), 0, Y + 2)
    block(planes(refs1, 1), range(1, Z - 1), 0, 1, 2)
    block(planes(refs1, 1), range(1, Z - 1), Y + 1, 1, 2)

    def between(refs, velocity, at_face, below, above):
        cross = dt * velocity[at_face]
        upward = cross > 0

        def donor(ref):
            return jnp.where(upward, ref[below], ref[above])

        return face_flux(cross, *[donor(ref) for ref in refs[3:]])

    def y_flux(z, y, kz, ky):
        rows = pl.ds(z, kz)
        face = (rows, pl.ds(y, ky))
        fy[face] = between(refs1, vy, face, face, (rows, pl.ds(y + 1, ky)))

    def y_update(z, y, kz, ky):
        rows = pl.ds(z, kz)
        low, high = pl.ds(y, ky), pl.ds(y + 1, ky)
        value = g1[pl.ds(z + 1, kz), pl.ds(y + 2, ky)]
        g2[pl.ds(z + 2, kz), pl.ds(y + 1, ky)] = (value - fy[rows, high] + fy[rows, low]) / (
            1.0 - dt * vy[rows, high] + dt * vy[rows, low]
        )

    halos2 = halo_copies(g2, spans_for(Y_SIDES + Z_SIDES, 2, 1), halo2_send, halo2_recv)
    block(y_flux, own, 0, 2)
    block(y_flux, own, Y - 1, 2)
    block(y_update, own, 0, 1, 2)
    block(y_update, own, Y - 1, 1, 2)
    for copy in halos2[:2]:
        copy.start()
    for zs in ((0, 1), (Z - 2, Z - 1)):
        block(y_flux, zs, 2, 2)
        block(y_flux, zs, 4, Y - 5)
        block(y_update, zs, 1, Y - 2)
    for copy in halos2[2:]:
        copy.start()
    block(y_flux, range(2, Z - 2), 2, 2)
    block(y_flux, range(2, Z - 2), 4, Y - 5)
    block(y_update, range(2, Z - 2), 1, Y - 2)

    block(smooths(refs2), range(2, Z + 2), 1, Y)
    block(planes(refs2, 0, 2), range(2, Z), 1, Y - 2)
    for copy in halos2[:2]:
        copy.wait()
    block(smooths(refs2), range(2, Z + 2), 0, 1)
    block(smooths(refs2), range(2, Z + 2), Y + 1, 1)
    block(planes(refs2, 0), range(2, Z), 0, 1, 2)
    block(planes(refs2, 0), range(2, Z), Y - 1, 1, 2)
    for copy in halos2[2:]:
        copy.wait()
    for zs in ((0, 1), (Z + 2, Z + 3)):
        block(smooths(refs2), zs, 0, Y + 2)
    for zs in ((0, 1), (Z, Z + 1)):
        block(planes(refs2, 0, 3), zs, 0, Y)

    def z_flux(z, y, kz, ky):
        face, above = (pl.ds(z, kz), pl.ds(y, ky)), (pl.ds(z + 1, kz), pl.ds(y, ky))
        fz[face] = between(refs2, vz, face, face, above)

    def z_fluxes(z):
        z_flux(z, 0, 1, Y // 2)
        z_flux(z, Y // 2, 1, Y - Y // 2)

    def z_update(z):
        for y in range(Y):
            value = (g2[z + 2, y + 1] - fz[z + 1, y] + fz[z, y]) / (
                1.0 - step_value * vz[z + 1, y] + step_value * vz[z, y]
            )
            out_ref[z, pl.ds(y, T, stride=Y), :] = value

    z_fluxes(0)
    loop(1, Z + 1, z_fluxes)
    loop(0, Z, z_update)


def writer(field_ref, step_ref, out_ref, dt_ref, sem):
    copy = pltpu.make_async_copy(field_ref, out_ref, sem)
    copy.start()
    dt_ref[0, 0] = step_ref[0, 0]
    copy.wait()


def solution(mesh):
    n_gy, n_gz = mesh.shape["gy"], mesh.shape["gz"]

    def shards(*blocks):
        Z, Y, X = blocks[0].shape
        T = X // LANES

        def split(block):
            return block.reshape(Z, Y, T, LANES).transpose(0, 2, 1, 3).reshape(Z, T * Y, LANES)

        def rows(*lead):
            return pltpu.VMEM((*lead, T, LANES), jnp.float32)

        dma = pltpu.SemaphoreType.DMA
        field, dt = pl.pallas_call(
            functools.partial(kernel, n_gy, n_gz),
            out_shape=(
                pltpu.VMEM((Z, T * Y, LANES), jnp.float32),
                pltpu.SMEM((1, 1), jnp.float32),
            ),
            in_specs=[pl.BlockSpec(memory_space=pltpu.HBM)] * 4,
            out_specs=(
                pl.BlockSpec(memory_space=pltpu.VMEM),
                pl.BlockSpec(memory_space=pltpu.SMEM),
            ),
            scratch_shapes=[
                *[pltpu.VMEM((Z, T * Y, LANES), jnp.float32)] * 4, dma((4,)),
                rows(Z + 2, Y + 2), rows(Z + 2, Y + 4), rows(Z + 4, Y + 2),
                *[rows(Z + 2, Y + 2)] * 2, *[rows(Z + 2, Y + 4)] * 2, *[rows(Z + 4, Y + 2)] * 2,
                *[rows(Z, Y)] * 4, *[rows(Z, Y + 2)] * 4, *[rows(Z + 2, Y)] * 4,
                rows(Z, Y), rows(Z, Y + 1), rows(Z + 1, Y), rows(Z, Y + 1), rows(Z + 1, Y),
                rows(n_gy), rows(n_gz),
                dma((8,)), dma((8,)), dma((10,)), dma((10,)), dma((8,)), dma((8,)),
                dma((2,)), dma((2,)),
                dma((n_gy - 1,)), dma((n_gy - 1,)), dma((n_gz - 1,)), dma((n_gz - 1,)),
            ],
            compiler_params=pltpu.CompilerParams(
                collective_id=0, has_side_effects=True, vmem_limit_bytes=66416640
            ),
        )(*[split(block) for block in blocks])
        field, dt = pl.pallas_call(
            writer,
            out_shape=(
                jax.ShapeDtypeStruct((Z, T * Y, LANES), jnp.float32),
                jax.ShapeDtypeStruct((1, 1), jnp.float32),
            ),
            in_specs=[
                pl.BlockSpec(memory_space=pltpu.VMEM),
                pl.BlockSpec(memory_space=pltpu.SMEM),
            ],
            out_specs=(
                pl.BlockSpec(memory_space=pltpu.HBM),
                pl.BlockSpec(memory_space=pltpu.SMEM),
            ),
            scratch_shapes=[dma],
        )(
            pltpu.with_memory_space_constraint(field, pltpu.VMEM),
            pltpu.with_memory_space_constraint(dt, pltpu.SMEM),
        )
        field = field.reshape(Z, T, Y, LANES).transpose(0, 2, 1, 3).reshape(Z, Y, X)
        return field, dt.reshape(())

    spec = P("gz", "gy", None)
    return jax.shard_map(
        shards, mesh=mesh, in_specs=(spec,) * 4, out_specs=(spec, P()), check_vma=False
    )
```

```python
import functools

import jax
import jax.numpy as jnp
from jax import lax
from jax.experimental import pallas as pl
from jax.experimental.pallas import tpu as pltpu
from jax.sharding import PartitionSpec as P

NEWTON = 5
CHUNKS = 4
LANES = 128
GROUP = 8

tilt_floor = 3.2
courant = 0.45
epsilon = 1e-06
tiny = 1e-30
tiny_unit = 1e-15

MESH = pl.DeviceIdType.MESH


def lane_of(value):
    return lax.broadcasted_iota(jnp.int32, value.shape, value.ndim - 1)


def x_next(value):
    turned = pltpu.roll(value, LANES - 1, value.ndim - 1)
    carried = pltpu.roll(turned, value.shape[-2] - 1, value.ndim - 2)
    return jnp.where(lane_of(value) == LANES - 1, carried, turned)


def x_prev(value):
    turned = pltpu.roll(value, 1, value.ndim - 1)
    carried = pltpu.roll(turned, 1, value.ndim - 2)
    return jnp.where(lane_of(value) == 0, carried, turned)


def solve_offset(g, tilt_a, tilt_b, tilt_d):
    volume = jnp.clip(g, 0.0, 1.0)
    lesser = jnp.minimum(volume, 1.0 - volume)
    low = jnp.minimum(tilt_a, tilt_b)
    high = jnp.maximum(tilt_a, tilt_b)
    unit = jnp.maximum(jnp.minimum(low, tilt_d), tiny_unit)
    middle = jnp.maximum(low, tilt_d)
    inverse = 1.0 / unit
    n2 = jnp.minimum(middle, high) * inverse
    n3 = jnp.maximum(middle, high) * inverse
    above = n2 + 1.0
    summed = above + n3
    product = n2 * n3
    target = product * (lesser + lesser)
    gap = 0.5 * jnp.maximum(above - n3, 0.0)
    offset = 0.5 * (summed - (product - target) / (n2 - gap * gap))
    for repeat in range(NEWTON - 1):
        p1 = jnp.minimum(offset, 1.0)
        q1 = offset - p1
        m2 = jnp.maximum(offset - n2, 0.0)
        p2 = jnp.minimum(m2, 1.0)
        q2 = m2 - p2
        p3 = jnp.maximum(offset - n3, 0.0)
        s1, s2, s3 = p1 * p1, p2 * p2, p3 * p3
        squares = s1 - s2 - s3
        cubes = s1 * p1 - s2 * p2 - s3 * p3
        q = q1 - q2
        rate = squares + (q + q)
        volume_part = cubes * (1.0 / 3.0) + q * (q1 + (q2 + 1.0))
        offset = offset - (volume_part - target) / rate
    return jnp.where(volume > 0.5, summed - offset, offset) * unit


def face_flux(cross, offset, tilt_a, tilt_b, slope):
    turn = slope * cross
    height = jnp.abs(turn)
    reach = offset - jnp.where(turn > 0, 0.0, jnp.abs(slope) - height)

    def parts(value):
        inside = jnp.maximum(value, 0.0)
        p = jnp.minimum(inside, height)
        q = inside - p
        return p * p * p, q * (q + height)

    reach_a = reach - tilt_a
    p0, q0 = parts(reach)
    p1, q1 = parts(reach_a)
    p2, q2 = parts(reach - tilt_b)
    p3, q3 = parts(reach_a - tilt_b)
    cubes = (p0 - p1) - (p2 - p3)
    wholes = (q0 - q1) - (q2 - q3)
    combo = cubes * ((1.0 / 3.0) / jnp.maximum(height, tiny)) + wholes
    return cross * combo / (2.0 * tilt_a * tilt_b)


def between(dt, planes, velocity, at_face, below, above):
    cross = dt * velocity[at_face]
    upward = cross > 0
    donor = [jnp.where(upward, ref[below], ref[above]) for ref in planes]
    return face_flux(cross, *donor)


def kernel(
    n_gy, n_gz, f_hbm, vx_hbm, vy_hbm, vz_hbm,
    g2, fz, vz, off2, ta2, tb2, sd2, step_ref, dt_ref,
    f_ref, vx_ref, vy_ref, vz_ref, load_sem,
    g0, g1, sx0, dx0, sx1, dx1, sx2, dx2,
    off0, ta0, tb0, sd0, off1, ta1, tb1, sd1,
    vx, vy, fy, part,
    halo0_send, halo0_recv, halo1_send, halo1_recv, halo2_send, halo2_recv,
    vel_send, vel_recv, part_sem,
):
    Z = f_ref.shape[0]
    T = sx0.shape[2]
    Y = f_ref.shape[1] // T
    loads = []
    for i, (source, target) in enumerate(
        ((f_hbm, f_ref), (vx_hbm, vx_ref), (vy_hbm, vy_ref), (vz_hbm, vz_ref))
    ):
        loads.append(pltpu.make_async_copy(source, target, load_sem.at[i]))
        loads[-1].start()
    my = lax.axis_index("gy")
    mz = lax.axis_index("gz")

    def at(dz, dy):
        return {
            "gy": lax.rem(my + dy + n_gy, n_gy),
            "gz": lax.rem(mz + dz + n_gz, n_gz),
        }

    barrier = pltpu.get_barrier_semaphore()
    greeted = [(a, b) for a in range(n_gz) for b in range(n_gy)][1:]
    for dz, dy in greeted:
        pl.semaphore_signal(barrier, inc=1, device_id=at(dz, dy), device_id_type=MESH)

    def rows_of(ref, z, y):
        return ref[z, pl.ds(y, T, stride=Y), :]

    def gather(low, high, body, carry):
        count = high - low
        grouped = max(u for u in range(1, GROUP + 1) if count % u == 0)

        def step(i, carry):
            for u in range(grouped):
                carry = body(low + i * grouped + u, carry)
            return carry
        return lax.fori_loop(0, count // grouped, step, carry)

    def loop(low, high, body):
        def step(i, carry):
            body(i)
            return carry
        gather(low, high, step, 0)

    def halo_copies(g, spans, sends, recvs):
        copies = []
        for index, (dz, dy, src_z, dst_z, src_y, dst_y) in enumerate(spans):
            copies.append(pltpu.make_async_remote_copy(
                src_ref=g.at[src_z, src_y],
                dst_ref=g.at[dst_z, dst_y],
                send_sem=sends.at[index],
                recv_sem=recvs.at[index],
                device_id=at(dz, dy),
                device_id_type=MESH,
            ))
        return copies

    def span(side, count, pad, depth):
        if side == 0:
            return pl.ds(pad, count), pl.ds(pad, count)
        if side > 0:
            return pl.ds(pad + count - depth, depth), pl.ds(pad - depth, depth)
        return pl.ds(pad, depth), pl.ds(pad + count, depth)

    def spans_for(sides, pad_z, pad_y):
        return [
            (dz, dy, *span(dz, Z, pad_z, pad_z), *span(dy, Y, pad_y, pad_y))
            for dz, dy in sides
        ]

    Y_SIDES = [(0, -1), (0, 1)]
    Z_SIDES = [(a, b) for a in (-1, 1) for b in (0, -1, 1)]

    def smooth_rows(g, sx, dx, z, y, kz, ky):
        value = g[pl.ds(z, kz), pl.ds(y, ky)]
        after, before = x_next(value), x_prev(value)
        sx[pl.ds(z, kz), pl.ds(y, ky)] = before + (value + value) + after
        dx[pl.ds(z, kz), pl.ds(y, ky)] = after - before

    def smooth_zero(arr):
        mid = arr[1:-1]
        return (arr[:-2] + mid) + (mid + arr[2:])

    def smooth_one(arr):
        pair = arr[:, :-1] + arr[:, 1:]
        return pair[:, :-1] + pair[:, 1:]

    def plane(refs, dim, z, y, kz, ky, parts=1):
        g, sx, dx, off, ta, tb, sd = refs
        s = sx[pl.ds(z, kz + 2), pl.ds(y, ky + 2)]
        d = dx[pl.ds(z, kz + 2), pl.ds(y, ky + 2)]
        grad_zero = smooth_one(s[2:] - s[:-2])
        across = smooth_zero(s)
        grad_one = (across[:, 2:] - across[:, :-2])
        grad_cells = smooth_one(smooth_zero(d))
        slopes = (grad_zero, grad_one, grad_cells)
        low = 0
        for part in range(parts):
            count = (ky - low) // (parts - part)
            cut = [value[:, low:low + count] for value in slopes]
            slope = cut[dim]
            tilt_a, tilt_b = [jnp.abs(cut[e]) + tilt_floor for e in range(3) if e != dim]
            value = g[pl.ds(z + 1, kz), pl.ds(y + 1 + low, count)]
            where = (pl.ds(z, kz), pl.ds(y + low, count))
            off[where] = solve_offset(value, tilt_a, tilt_b, jnp.abs(slope))
            ta[where] = tilt_a
            tb[where] = tilt_b
            sd[where] = slope
            low += count

    def block(body, zs, y, ky, kz=1):
        count = len(zs) // kz
        step = zs[1] - zs[0] if len(zs) > 1 else 1
        loop(0, count, lambda i: body(zs[0] + step * kz * i, y, kz, ky))

    def both(body, zs, ys, kz=2):
        count = len(zs) // kz

        def step(i):
            for y in ys:
                body(zs[0] + kz * i, y, kz, 1)
        loop(0, count, step)

    def planes(refs, dim, parts=1):
        return lambda z, y, kz, ky: plane(refs, dim, z, y, kz, ky, parts)

    def smooths(refs):
        return lambda z, y, kz, ky: smooth_rows(refs[0], refs[1], refs[2], z, y, kz, ky)

    own = range(0, Z)
    refs0 = (g0, sx0, dx0, off0, ta0, tb0, sd0)
    refs1 = (g1, sx1, dx1, off1, ta1, tb1, sd1)
    refs2 = (g2, sx2, dx2, off2, ta2, tb2, sd2)

    def donors(z, y, kz, ky):
        where = (pl.ds(z, kz), pl.ds(y, ky))
        upward = vx[where] > 0
        for ref in (off0, ta0, tb0, sd0):
            value = ref[where]
            ref[where] = jnp.where(upward, value, x_next(value))

    def donors_in():
        loop(1, Z - 1, lambda z: donors(z, 1, 1, Y - 2))

    def donors_edge():
        for y in (0, Y - 1):
            block(donors, own, y, 1, 4)
        for z in (0, Z - 1):
            donors(z, 1, 1, Y - 2)

    def ghost_rows(refs, spans):
        for z, y, kz, ky in spans:
            smooth_rows(*refs[:3], z, y, kz, ky)

    def fill(z, total):
        for y in range(Y):
            f = rows_of(f_ref, z, y)
            g0[z + 1, y + 1] = f
            total = total + 4.0 * f * (1.0 - f)
        return total

    loads[0].wait()
    total = gather(0, Z, fill, jnp.zeros((T, LANES), jnp.float32))

    def fill_velocity(z, peak):
        for y in range(Y):
            a = rows_of(vx_ref, z, y)
            b = rows_of(vy_ref, z, y)
            c = rows_of(vz_ref, z, y)
            vx[z, y] = a
            vy[z, y + 1] = b
            vz[z + 1, y] = c
            peak = jnp.maximum(peak, jnp.maximum(jnp.abs(a), jnp.maximum(jnp.abs(b), jnp.abs(c))))
        return peak

    for copy in loads[1:]:
        copy.wait()
    peak = gather(0, Z, fill_velocity, jnp.zeros((T, LANES), jnp.float32))
    low_lanes = lane_of(jnp.zeros((1, LANES), jnp.float32)) < LANES // 2

    def folded(sums, peaks):
        sums = jnp.sum(sums, axis=0, keepdims=True)
        peaks = jnp.max(peaks, axis=0, keepdims=True)
        sums = sums + pltpu.roll(sums, LANES // 2, 1)
        peaks = jnp.maximum(peaks, pltpu.roll(peaks, LANES // 2, 1))
        return jnp.where(low_lanes, sums, peaks)

    me = mz * n_gy + my
    part[me] = folded(total, peak)
    pl.semaphore_wait(barrier, len(greeted))
    vel_copies = [
        pltpu.make_async_remote_copy(
            src_ref=vy.at[:, pl.ds(Y, 1)], dst_ref=vy.at[:, pl.ds(0, 1)],
            send_sem=vel_send.at[0], recv_sem=vel_recv.at[0],
            device_id=at(0, 1), device_id_type=MESH,
        ),
        pltpu.make_async_remote_copy(
            src_ref=vz.at[pl.ds(Z, 1)], dst_ref=vz.at[pl.ds(0, 1)],
            send_sem=vel_send.at[1], recv_sem=vel_recv.at[1],
            device_id=at(1, 0), device_id_type=MESH,
        ),
    ]

    part_copies = [
        pltpu.make_async_remote_copy(
            src_ref=part.at[me], dst_ref=part.at[me],
            send_sem=part_sem.at[0], recv_sem=part_sem.at[1],
            device_id=at(*away), device_id_type=MESH,
        )
        for away in greeted
    ]
    for copy in part_copies:
        copy.start()
    halos0 = halo_copies(g0, spans_for(Y_SIDES + Z_SIDES, 1, 1), halo0_send, halo0_recv)
    for copy in halos0:
        copy.start()

    block(smooths(refs0), range(1, Z + 1), 1, Y)
    block(planes(refs0, 2, 2), range(1, Z - 1), 1, Y - 2)
    donors_in()
    for copy in halos0:
        copy.wait()
    for copy in vel_copies:
        copy.start()
    ghost_rows(refs0, [
        (0, 0, 1, Y + 2), (Z + 1, 0, 1, Y + 2), (1, 0, Z, 1), (1, Y + 1, Z, 1)
    ])
    both(planes(refs0, 2), own, (0, Y - 1))
    block(planes(refs0, 2, 2), (0, Z - 1), 1, Y - 2)

    donors_edge()
    others = pl.ds(0, len(greeted))
    arrived = pltpu.make_async_remote_copy(
        src_ref=part.at[others], dst_ref=part.at[others],
        send_sem=part_sem.at[0], recv_sem=part_sem.at[1],
        device_id=at(*greeted[0]), device_id_type=MESH,
    )
    arrived.wait()
    sums = peaks = part[0]
    for i in range(1, n_gy * n_gz):
        sums = sums + part[i]
        peaks = jnp.maximum(peaks, part[i])
    sums = jnp.where(low_lanes, sums, 0.0)
    peaks = jnp.where(low_lanes, 0.0, peaks)
    cells_all = float(Z * Y * T * LANES * n_gy * n_gz)
    share = jnp.broadcast_to(jnp.sum(sums, keepdims=True), (T, LANES)) / cells_all
    umax = jnp.broadcast_to(jnp.max(peaks, keepdims=True), (T, LANES))
    step_value = courant / ((umax + epsilon) * (1.0 + share))
    dt_ref[0, 0] = jnp.max(step_value)
    step_ref[...] = step_value
    dt = step_value[None, None]

    def x_update(z, y, kz, ky):
        where = (pl.ds(z, kz), pl.ds(y, ky))
        cross = dt * vx[where]
        flux = face_flux(cross, off0[where], ta0[where], tb0[where], sd0[where])
        value = g0[pl.ds(z + 1, kz), pl.ds(y + 1, ky)]
        g1[pl.ds(z + 1, kz), pl.ds(y + 2, ky)] = (value - flux + x_prev(flux)) / (
            1.0 - cross + x_prev(cross)
        )

    def y_flux(z, y, kz, ky):
        rows = pl.ds(z, kz)
        face = (rows, pl.ds(y, ky))
        fy[face] = between(dt, refs1[3:], vy, face, face, (rows, pl.ds(y + 1, ky)))

    def y_update(z, y, kz, ky):
        rows = pl.ds(z, kz)
        low, high = pl.ds(y, ky), pl.ds(y + 1, ky)
        value = g1[pl.ds(z + 1, kz), pl.ds(y + 2, ky)]
        g2[pl.ds(z + 2, kz), pl.ds(y + 1, ky)] = (value - fy[rows, high] + fy[rows, low]) / (
            1.0 - dt * vy[rows, high] + dt * vy[rows, low]
        )

    deep = spans_for([(a, b) for a in (-1, 1) for b in (-1, 1)], 1, 2)
    spans1 = []
    for depth in (1, 2):
        for dy in (-1, 1):
            src, dst = span(dy, Y, 2, 2)
            near = (0, 1)[(dy > 0) == (depth == 1)]
            spans1.append((
                0, dy, pl.ds(1, Z), pl.ds(1, Z),
                pl.ds(src.start + near, 1), pl.ds(dst.start + near, 1),
            ))
    for dz in (-1, 1):
        spans1.append((dz, 0, *span(dz, Z, 1, 1), pl.ds(2, Y), pl.ds(2, Y)))
    spans1 += deep
    halos1 = halo_copies(g1, spans1, halo1_send, halo1_recv)

    both(x_update, own, (0, Y - 1))
    for copy in halos1[:2]:
        copy.start()
    both(x_update, own, (1, Y - 2))
    for copy in halos1[2:4]:
        copy.start()
    block(x_update, (0, Z - 1), 2, Y - 4)
    for copy in halos1[4:]:
        copy.start()
    block(x_update, range(1, Z - 1), 2, Y - 4)
    block(smooths(refs1), range(1, Z + 1), 2, Y)
    block(planes(refs1, 1, 2), range(1, Z - 1), 2, Y - 2)
    block(y_flux, range(1, Z - 1), 2, 2)
    block(y_flux, range(1, Z - 1), 4, Y - 5)
    for copy in vel_copies:
        copy.wait()
    for copy in halos1[:2]:
        copy.wait()
    ghost_rows(refs1, [(1, 1, Z, 1), (1, Y + 2, Z, 1)])
    both(planes(refs1, 1), range(1, Z - 1), (1, Y))
    for copy in halos1[2:]:
        copy.wait()
    ghost_rows(refs1, [
        (0, 0, 1, Y + 4), (Z + 1, 0, 1, Y + 4), (1, 0, Z, 1), (1, Y + 3, Z, 1)
    ])
    block(planes(refs1, 1, 3), (0, Z - 1), 0, Y + 2)
    both(planes(refs1, 1), range(1, Z - 1), (0, Y + 1))

    halos2 = halo_copies(g2, spans_for(Y_SIDES + Z_SIDES, 2, 1), halo2_send, halo2_recv)
    both_faces = lambda z, y, kz, ky: (y_flux(z, 0, kz, 2), y_flux(z, Y - 1, kz, 2))
    block(both_faces, own, 0, 2)
    both(y_update, own, (0, Y - 1))
    for copy in halos2[:2]:
        copy.start()
    block(y_flux, (0, Z - 1), 2, 2)
    block(y_flux, (0, Z - 1), 4, Y - 5)
    for zs in ((0, 1), (Z - 2, Z - 1)):
        block(y_update, zs, 1, Y - 2)
    for copy in halos2[2:]:
        copy.start()
    block(y_update, range(2, Z - 2), 1, Y - 2)

    block(smooths(refs2), range(2, Z + 2), 1, Y)
    block(planes(refs2, 0, 2), range(2, Z), 1, Y - 2)

    def z_flux(z):
        for y in (1, Y // 2):
            face, above = (pl.ds(z, 1), pl.ds(y, 3)), (pl.ds(z + 1, 1), pl.ds(y, 3))
            fz[face] = between(dt, refs2[3:], vz, face, face, above)

    loop(2, Z - 1, z_flux)
    for copy in halos2[:2]:
        copy.wait()
    ghost_rows(refs2, [(2, 0, Z, 1), (2, Y + 1, Z, 1)])
    both(planes(refs2, 0), range(2, Z), (0, Y - 1))
    for copy in halos2[2:]:
        copy.wait()
    ghost_rows(refs2, [(0, 0, 2, Y + 2), (Z + 2, 0, 2, Y + 2)])
    for zs in ((0, 1), (Z, Z + 1)):
        block(planes(refs2, 0, 3), zs, 0, Y)


def finish(
    g2, fz_in, vz, off, ta, tb, sd, step_ref, dt_in, out_hbm, dt_ref, fz, field, sems
):
    Z, Y, T = fz_in.shape[0] - 1, *fz_in.shape[1:3]
    dt_ref[0, 0] = dt_in[0, 0]
    step = step_ref[...]
    dt = step[None, None]
    per = Z // CHUNKS
    copies = []

    def flux(z, y, kz, ky):
        face, above = (pl.ds(z, kz), pl.ds(y, ky)), (pl.ds(z + 1, kz), pl.ds(y, ky))
        fz[face] = between(dt, (off, ta, tb, sd), vz, face, face, above)

    done = 0
    for chunk in range(CHUNKS):
        low, high = chunk * per, (chunk + 1) * per
        for z in range(done, high + 1):
            if 2 <= z < Z - 1:
                flux(z, 0, 1, 1)
                flux(z, Y - 1, 1, 1)
                fz[z, pl.ds(1, Y - 2)] = fz_in[z, pl.ds(1, Y - 2)]
            else:
                flux(z, 0, 1, Y // 2)
                flux(z, Y // 2, 1, Y - Y // 2)
        done = high + 1
        for z in range(low, high):
            for y in range(Y):
                value = (g2[z + 2, y + 1] - fz[z + 1, y] + fz[z, y]) / (
                    1.0 - step * vz[z + 1, y] + step * vz[z, y]
                )
                field[z, pl.ds(y, T, stride=Y), :] = value
        part = pl.ds(low, per)
        copies.append(pltpu.make_async_copy(field.at[part], out_hbm.at[part], sems.at[chunk]))
        copies[-1].start()
    for copy in copies:
        copy.wait()


def solution(mesh):
    n_gy, n_gz = mesh.shape["gy"], mesh.shape["gz"]

    def shards(*blocks):
        Z, Y, X = blocks[0].shape
        T = X // LANES

        def split(block):
            return block.reshape(Z, Y, T, LANES).transpose(0, 2, 1, 3).reshape(Z, T * Y, LANES)

        def rows(*lead):
            return pltpu.VMEM((*lead, T, LANES), jnp.float32)

        dma = pltpu.SemaphoreType.DMA
        in_vmem = pl.BlockSpec(memory_space=pltpu.VMEM)
        in_smem = pl.BlockSpec(memory_space=pltpu.SMEM)
        kept = (
            rows(Z + 4, Y + 2), rows(Z + 1, Y), rows(Z + 1, Y), *[rows(Z + 2, Y)] * 4
        )
        *state, dt = pl.pallas_call(
            functools.partial(kernel, n_gy, n_gz),
            out_shape=(
                *kept, pltpu.VMEM((T, LANES), jnp.float32), pltpu.SMEM((1, 1), jnp.float32),
            ),
            in_specs=[pl.BlockSpec(memory_space=pltpu.HBM)] * 4,
            out_specs=(*[in_vmem] * (len(kept) + 1), in_smem),
            scratch_shapes=[
                *[pltpu.VMEM((Z, T * Y, LANES), jnp.float32)] * 4, dma((4,)),
                rows(Z + 2, Y + 2), rows(Z + 2, Y + 4),
                *[rows(Z + 2, Y + 2)] * 2, *[rows(Z + 2, Y + 4)] * 2, *[rows(Z + 4, Y + 2)] * 2,
                *[rows(Z, Y)] * 4, *[rows(Z, Y + 2)] * 4,
                rows(Z, Y), rows(Z, Y + 1), rows(Z, Y + 1),
                pltpu.VMEM((n_gy * n_gz, 1, LANES), jnp.float32),
                dma((8,)), dma((8,)), dma((10,)), dma((10,)), dma((8,)), dma((8,)),
                dma((2,)), dma((2,)),
                dma((2,)),
            ],
            compiler_params=pltpu.CompilerParams(
                collective_id=0, has_side_effects=True, vmem_limit_bytes=62640128
            ),
        )(*[split(block) for block in blocks])
        field, dt = pl.pallas_call(
            finish,
            out_shape=(
                jax.ShapeDtypeStruct((Z, T * Y, LANES), jnp.float32),
                jax.ShapeDtypeStruct((1, 1), jnp.float32),
            ),
            in_specs=[*[in_vmem] * len(state), in_smem],
            out_specs=(pl.BlockSpec(memory_space=pltpu.HBM), in_smem),
            scratch_shapes=[
                rows(Z + 1, Y), pltpu.VMEM((Z, T * Y, LANES), jnp.float32), dma((CHUNKS,)),
            ],
            compiler_params=pltpu.CompilerParams(vmem_limit_bytes=16777216),
        )(
            *[pltpu.with_memory_space_constraint(value, pltpu.VMEM) for value in state],
            pltpu.with_memory_space_constraint(dt, pltpu.SMEM),
        )
        field = field.reshape(Z, T, Y, LANES).transpose(0, 2, 1, 3).reshape(Z, Y, X)
        return field, dt.reshape(())

    spec = P("gz", "gy", None)
    return jax.shard_map(
        shards, mesh=mesh, in_specs=(spec,) * 4, out_specs=(spec, P()), check_vma=False
    )
```

```python
import functools

import jax
import jax.numpy as jnp
from jax import lax
from jax.experimental import pallas as pl
from jax.experimental.pallas import tpu as pltpu
from jax.sharding import PartitionSpec as P

NEWTON = 5
CHUNKS = 4
HALVES = 2
LANES = 128
GROUP = 8

tilt_floor = 3.2
courant = 0.45
epsilon = 1e-06
tiny = 1e-30
tiny_unit = 1e-15

MESH = pl.DeviceIdType.MESH


def lane_of(value):
    return lax.broadcasted_iota(jnp.int32, value.shape, value.ndim - 1)


def x_next(value):
    turned = pltpu.roll(value, LANES - 1, value.ndim - 1)
    carried = pltpu.roll(turned, value.shape[-2] - 1, value.ndim - 2)
    return jnp.where(lane_of(value) == LANES - 1, carried, turned)


def x_prev(value):
    turned = pltpu.roll(value, 1, value.ndim - 1)
    carried = pltpu.roll(turned, 1, value.ndim - 2)
    return jnp.where(lane_of(value) == 0, carried, turned)


def solve_offset(g, tilt_a, tilt_b, tilt_d):
    volume = jnp.clip(g, 0.0, 1.0)
    lesser = jnp.minimum(volume, 1.0 - volume)
    low = jnp.minimum(tilt_a, tilt_b)
    high = jnp.maximum(tilt_a, tilt_b)
    unit = jnp.maximum(jnp.minimum(low, tilt_d), tiny_unit)
    middle = jnp.maximum(low, tilt_d)
    inverse = 1.0 / unit
    n2 = jnp.minimum(middle, high) * inverse
    n3 = jnp.maximum(middle, high) * inverse
    above = n2 + 1.0
    summed = above + n3
    product = n2 * n3
    target = product * (lesser + lesser)
    gap = 0.5 * jnp.maximum(above - n3, 0.0)
    offset = 0.5 * (summed - (product - target) / (n2 - gap * gap))
    for repeat in range(NEWTON - 1):
        p1 = jnp.minimum(offset, 1.0)
        q1 = offset - p1
        m2 = jnp.maximum(offset - n2, 0.0)
        p2 = jnp.minimum(m2, 1.0)
        q2 = m2 - p2
        p3 = jnp.maximum(offset - n3, 0.0)
        s1, s2, s3 = p1 * p1, p2 * p2, p3 * p3
        squares = s1 - s2 - s3
        cubes = s1 * p1 - s2 * p2 - s3 * p3
        q = q1 - q2
        rate = squares + (q + q)
        volume_part = cubes * (1.0 / 3.0) + q * (q1 + (q2 + 1.0))
        offset = offset - (volume_part - target) / rate
    return jnp.where(volume > 0.5, summed - offset, offset) * unit


def face_flux(cross, offset, tilt_a, tilt_b, slope):
    turn = slope * cross
    height = jnp.abs(turn)
    reach = offset - jnp.where(turn > 0, 0.0, jnp.abs(slope) - height)

    def parts(value):
        inside = jnp.maximum(value, 0.0)
        p = jnp.minimum(inside, height)
        q = inside - p
        return p * p * p, q * (q + height)

    reach_a = reach - tilt_a
    p0, q0 = parts(reach)
    p1, q1 = parts(reach_a)
    p2, q2 = parts(reach - tilt_b)
    p3, q3 = parts(reach_a - tilt_b)
    cubes = (p0 - p1) - (p2 - p3)
    wholes = (q0 - q1) - (q2 - q3)
    combo = cubes * ((1.0 / 3.0) / jnp.maximum(height, tiny)) + wholes
    return cross * combo / (2.0 * tilt_a * tilt_b)


def between(dt, planes, velocity, at_face, below, above):
    cross = dt * velocity[at_face]
    upward = cross > 0
    donor = [jnp.where(upward, ref[below], ref[above]) for ref in planes]
    return face_flux(cross, *donor)


def kernel(
    n_gy, n_gz, f_hbm, vx_hbm, vy_hbm, vz_hbm,
    middle, g2, vz, off2, ta2, tb2, sd2, step_ref, dt_ref,
    f_ref, vx_ref, vy_ref, vz_ref, load_sem,
    g0, g1, sx0, dx0, sx1, dx1, sx2, dx2,
    off0, ta0, tb0, sd0, off1, ta1, tb1, sd1,
    vx, vy, fy, fz, part,
    halo0_send, halo0_recv, halo1_send, halo1_recv, halo2_send, halo2_recv,
    vel_send, vel_recv, part_sem,
):
    Z = f_ref.shape[0]
    T = sx0.shape[2]
    Y = f_ref.shape[1] // T
    loads = []
    for i, (source, target) in enumerate(
        ((f_hbm, f_ref), (vx_hbm, vx_ref), (vy_hbm, vy_ref), (vz_hbm, vz_ref))
    ):
        loads.append(pltpu.make_async_copy(source, target, load_sem.at[i]))
        loads[-1].start()
    my = lax.axis_index("gy")
    mz = lax.axis_index("gz")

    def at(dz, dy):
        return {
            "gy": lax.rem(my + dy + n_gy, n_gy),
            "gz": lax.rem(mz + dz + n_gz, n_gz),
        }

    barrier = pltpu.get_barrier_semaphore()
    greeted = [(a, b) for a in range(n_gz) for b in range(n_gy)][1:]
    for dz, dy in greeted:
        pl.semaphore_signal(barrier, inc=1, device_id=at(dz, dy), device_id_type=MESH)

    def rows_of(ref, z, y):
        return ref[z, pl.ds(y, T, stride=Y), :]

    def gather(low, high, body, carry, most=GROUP):
        count = high - low
        grouped = max(u for u in range(1, most + 1) if count % u == 0)

        def step(i, carry):
            for u in range(grouped):
                carry = body(low + i * grouped + u, carry)
            return carry
        return lax.fori_loop(0, count // grouped, step, carry)

    def loop(low, high, body, most=GROUP):
        def step(i, carry):
            body(i)
            return carry
        gather(low, high, step, 0, most)

    def halo_copies(g, spans, sends, recvs):
        copies = []
        for index, (dz, dy, src_z, dst_z, src_y, dst_y) in enumerate(spans):
            copies.append(pltpu.make_async_remote_copy(
                src_ref=g.at[src_z, src_y],
                dst_ref=g.at[dst_z, dst_y],
                send_sem=sends.at[index],
                recv_sem=recvs.at[index],
                device_id=at(dz, dy),
                device_id_type=MESH,
            ))
        return copies

    def span(side, count, pad, depth):
        if side == 0:
            return pl.ds(pad, count), pl.ds(pad, count)
        if side > 0:
            return pl.ds(pad + count - depth, depth), pl.ds(pad - depth, depth)
        return pl.ds(pad, depth), pl.ds(pad + count, depth)

    def spans_for(sides, pad_z, pad_y):
        return [
            (dz, dy, *span(dz, Z, pad_z, pad_z), *span(dy, Y, pad_y, pad_y))
            for dz, dy in sides
        ]

    Y_SIDES = [(0, -1), (0, 1)]
    Z_SIDES = [(-1, 0), (1, 0)]
    CORNERS = [(a, b) for a in (-1, 1) for b in (-1, 1)]

    def smooth_rows(g, sx, dx, z, y, kz, ky):
        value = g[pl.ds(z, kz), pl.ds(y, ky)]
        after, before = x_next(value), x_prev(value)
        sx[pl.ds(z, kz), pl.ds(y, ky)] = before + (value + value) + after
        dx[pl.ds(z, kz), pl.ds(y, ky)] = after - before

    def smooth_zero(arr):
        mid = arr[1:-1]
        return (arr[:-2] + mid) + (mid + arr[2:])

    def smooth_one(arr):
        pair = arr[:, :-1] + arr[:, 1:]
        return pair[:, :-1] + pair[:, 1:]

    def plane(refs, dim, z, y, kz, ky, parts=1):
        g, sx, dx, off, ta, tb, sd = refs
        s = sx[pl.ds(z, kz + 2), pl.ds(y, ky + 2)]
        d = dx[pl.ds(z, kz + 2), pl.ds(y, ky + 2)]
        grad_zero = smooth_one(s[2:] - s[:-2])
        across = smooth_zero(s)
        grad_one = (across[:, 2:] - across[:, :-2])
        grad_cells = smooth_one(smooth_zero(d))
        slopes = (grad_zero, grad_one, grad_cells)
        low = 0
        for part in range(parts):
            count = (ky - low) // (parts - part)
            cut = [value[:, low:low + count] for value in slopes]
            slope = cut[dim]
            tilt_a, tilt_b = [jnp.abs(cut[e]) + tilt_floor for e in range(3) if e != dim]
            value = g[pl.ds(z + 1, kz), pl.ds(y + 1 + low, count)]
            where = (pl.ds(z, kz), pl.ds(y + low, count))
            off[where] = solve_offset(value, tilt_a, tilt_b, jnp.abs(slope))
            ta[where] = tilt_a
            tb[where] = tilt_b
            sd[where] = slope
            low += count

    def block(body, zs, y, ky, kz=1):
        count = len(zs) // kz
        step = zs[1] - zs[0] if len(zs) > 1 else 1
        loop(0, count, lambda i: body(zs[0] + step * kz * i, y, kz, ky))

    def both(body, zs, ys, kz=2):
        count = len(zs) // kz

        def step(i):
            for y in ys:
                body(zs[0] + kz * i, y, kz, 1)
        loop(0, count, step)

    def planes(refs, dim, parts=1):
        return lambda z, y, kz, ky: plane(refs, dim, z, y, kz, ky, parts)

    def smooth_own(refs, z, y):
        loop(z, z + Z, lambda i: smooth_rows(*refs[:3], i, y, 1, Y), Z)

    own = range(0, Z)
    refs0 = (g0, sx0, dx0, off0, ta0, tb0, sd0)
    refs1 = (g1, sx1, dx1, off1, ta1, tb1, sd1)
    refs2 = (g2, sx2, dx2, off2, ta2, tb2, sd2)

    def donors(z, y, kz, ky):
        where = (pl.ds(z, kz), pl.ds(y, ky))
        upward = vx[where] > 0
        for ref in (off0, ta0, tb0, sd0):
            value = ref[where]
            ref[where] = jnp.where(upward, value, x_next(value))

    def donors_in():
        loop(1, Z - 1, lambda z: donors(z, 1, 1, Y - 2))

    def ghost_rows(refs, spans):
        for z, y, kz, ky in spans:
            smooth_rows(*refs[:3], z, y, kz, ky)

    def fill(z, total):
        for y in range(Y):
            f = rows_of(f_ref, z, y)
            g0[z + 1, y + 1] = f
            total = total + 4.0 * f * (1.0 - f)
        return total

    loads[0].wait()
    total = gather(0, Z, fill, jnp.zeros((T, LANES), jnp.float32))

    def fill_velocity(z, peak):
        for y in range(Y):
            a = rows_of(vx_ref, z, y)
            b = rows_of(vy_ref, z, y)
            c = rows_of(vz_ref, z, y)
            vx[z, y] = a
            vy[z, y + 1] = b
            vz[z + 1, y] = c
            peak = jnp.maximum(peak, jnp.maximum(jnp.abs(a), jnp.maximum(jnp.abs(b), jnp.abs(c))))
        return peak

    for copy in loads[1:]:
        copy.wait()
    peak = gather(0, Z, fill_velocity, jnp.zeros((T, LANES), jnp.float32))
    low_lanes = lane_of(jnp.zeros((1, LANES), jnp.float32)) < LANES // 2

    def folded(sums, peaks):
        sums = jnp.sum(sums, axis=0, keepdims=True)
        peaks = jnp.max(peaks, axis=0, keepdims=True)
        sums = sums + pltpu.roll(sums, LANES // 2, 1)
        peaks = jnp.maximum(peaks, pltpu.roll(peaks, LANES // 2, 1))
        return jnp.where(low_lanes, sums, peaks)

    me = mz * n_gy + my
    part[me] = folded(total, peak)
    pl.semaphore_wait(barrier, len(greeted))
    vel_copies = [
        pltpu.make_async_remote_copy(
            src_ref=vy.at[:, pl.ds(Y, 1)], dst_ref=vy.at[:, pl.ds(0, 1)],
            send_sem=vel_send.at[0], recv_sem=vel_recv.at[0],
            device_id=at(0, 1), device_id_type=MESH,
        ),
        pltpu.make_async_remote_copy(
            src_ref=vz.at[pl.ds(Z, 1)], dst_ref=vz.at[pl.ds(0, 1)],
            send_sem=vel_send.at[1], recv_sem=vel_recv.at[1],
            device_id=at(1, 0), device_id_type=MESH,
        ),
    ]

    halos0 = halo_copies(
        g0, spans_for(Y_SIDES + Z_SIDES + CORNERS, 1, 1), halo0_send, halo0_recv
    )
    for copy in halos0:
        copy.start()
    part_copies = [
        pltpu.make_async_remote_copy(
            src_ref=part.at[me], dst_ref=part.at[me],
            send_sem=part_sem.at[0], recv_sem=part_sem.at[1],
            device_id=at(*away), device_id_type=MESH,
        )
        for away in greeted
    ]
    for copy in part_copies:
        copy.start()

    smooth_own(refs0, 1, 1)
    block(planes(refs0, 2, 2), range(1, Z - 1), 1, Y - 2)
    donors_in()
    for copy in halos0[2:4]:
        copy.wait()
    ghost_rows(refs0, [(0, 1, 1, Y), (Z + 1, 1, 1, Y)])
    block(planes(refs0, 2, 2), (0, Z - 1), 1, Y - 2)
    for z in (0, Z - 1):
        donors(z, 1, 1, Y - 2)
    for copy in halos0[:2] + halos0[4:]:
        copy.wait()
    for copy in vel_copies:
        copy.start()
    ghost_rows(refs0, [(0, 0, Z + 2, 1), (0, Y + 1, Z + 2, 1)])
    both(planes(refs0, 2), own, (0, Y - 1))
    both(donors, own, (0, Y - 1), 4)
    others = pl.ds(0, len(greeted))
    arrived = pltpu.make_async_remote_copy(
        src_ref=part.at[others], dst_ref=part.at[others],
        send_sem=part_sem.at[0], recv_sem=part_sem.at[1],
        device_id=at(*greeted[0]), device_id_type=MESH,
    )
    arrived.wait()
    sums = peaks = part[0]
    for i in range(1, n_gy * n_gz):
        sums = sums + part[i]
        peaks = jnp.maximum(peaks, part[i])
    sums = jnp.where(low_lanes, sums, 0.0)
    peaks = jnp.where(low_lanes, 0.0, peaks)
    cells_all = float(Z * Y * T * LANES * n_gy * n_gz)
    share = jnp.broadcast_to(jnp.sum(sums, keepdims=True), (T, LANES)) / cells_all
    umax = jnp.broadcast_to(jnp.max(peaks, keepdims=True), (T, LANES))
    step_value = courant / ((umax + epsilon) * (1.0 + share))
    dt_ref[0, 0] = jnp.max(step_value)
    step_ref[...] = step_value
    dt = step_value[None, None]

    def x_update(z, y, kz, ky):
        where = (pl.ds(z, kz), pl.ds(y, ky))
        cross = dt * vx[where]
        flux = face_flux(cross, off0[where], ta0[where], tb0[where], sd0[where])
        value = g0[pl.ds(z + 1, kz), pl.ds(y + 1, ky)]
        g1[pl.ds(z + 1, kz), pl.ds(y + 2, ky)] = (value - flux + x_prev(flux)) / (
            1.0 - cross + x_prev(cross)
        )

    def y_flux(z, y, kz, ky):
        rows = pl.ds(z, kz)
        face = (rows, pl.ds(y, ky))
        fy[face] = between(dt, refs1[3:], vy, face, face, (rows, pl.ds(y + 1, ky)))

    def y_update(z, y, kz, ky):
        rows = pl.ds(z, kz)
        low, high = pl.ds(y, ky), pl.ds(y + 1, ky)
        value = g1[pl.ds(z + 1, kz), pl.ds(y + 2, ky)]
        g2[pl.ds(z + 2, kz), pl.ds(y + 1, ky)] = (value - fy[rows, high] + fy[rows, low]) / (
            1.0 - dt * vy[rows, high] + dt * vy[rows, low]
        )

    spans1 = []
    for depth in (1, 2):
        for low in range(0, Z, Z // HALVES):
            for dy in (-1, 1):
                src, dst = span(dy, Y, 2, 2)
                near = (0, 1)[(dy > 0) == (depth == 1)]
                rows = pl.ds(1 + low, Z // HALVES)
                spans1.append((
                    0, dy, rows, rows,
                    pl.ds(src.start + near, 1), pl.ds(dst.start + near, 1),
                ))
    deep = len(spans1)
    for dz in (-1, 1):
        spans1.append((dz, 0, *span(dz, Z, 1, 1), pl.ds(2, Y), pl.ds(2, Y)))
    spans1 += spans_for(CORNERS, 1, 2)
    halos1 = halo_copies(g1, spans1, halo1_send, halo1_recv)
    first = halos1[:deep // 2]
    second = halos1[deep // 2:deep]
    flat, corners = halos1[deep:deep + 2], halos1[deep + 2:]

    for copies, ys in ((first, (0, Y - 1)), (second, (1, Y - 2))):
        for part_of in range(HALVES):
            low = part_of * (Z // HALVES)
            both(x_update, range(low, low + Z // HALVES), ys)
            for copy in copies[2 * part_of:2 * part_of + 2]:
                copy.start()
    block(x_update, (0, Z - 1), 2, Y - 4)
    for copy in flat + corners:
        copy.start()
    block(x_update, range(1, Z - 1), 2, Y - 4)
    smooth_own(refs1, 1, 2)
    block(planes(refs1, 1, 2), range(1, Z - 1), 2, Y - 2)
    for copy in flat:
        copy.wait()
    ghost_rows(refs1, [(0, 2, 1, Y), (Z + 1, 2, 1, Y)])
    block(planes(refs1, 1, 2), (0, Z - 1), 2, Y - 2)
    block(y_flux, own, 2, 2)
    block(y_flux, own, 4, Y - 5)
    for copy in vel_copies:
        copy.wait()
    for copy in first:
        copy.wait()
    ghost_rows(refs1, [(1, 1, Z, 1), (1, Y + 2, Z, 1)])
    both(planes(refs1, 1), range(1, Z - 1), (1, Y))
    for copy in second + corners:
        copy.wait()
    ghost_rows(refs1, [
        (1, 0, Z, 1), (1, Y + 3, Z, 1),
        (0, 0, 1, 2), (0, Y + 2, 1, 2), (Z + 1, 0, 1, 2), (Z + 1, Y + 2, 1, 2),
    ])
    for z in (0, Z - 1):
        plane(refs1, 1, z, 0, 1, 2)
        plane(refs1, 1, z, Y, 1, 2)

    per = Z // CHUNKS
    spans2 = []
    for low in range(0, Z, per):
        for dy in (-1, 1):
            rows = pl.ds(2 + low, per)
            spans2.append((0, dy, rows, rows, *span(dy, Y, 1, 1)))
    spans2 += spans_for(Z_SIDES + CORNERS, 2, 1)
    halos2 = halo_copies(g2, spans2, halo2_send, halo2_recv)
    side, flat, corners = halos2[:2 * CHUNKS], halos2[2 * CHUNKS:-4], halos2[-4:]

    for chunk in (0, CHUNKS - 1, *range(1, CHUNKS - 1)):
        low, high = chunk * per, (chunk + 1) * per
        start, count = max(low, 1), min(high, Z - 1) - max(low, 1)
        for y in (0, Y + 1):
            plane(refs1, 1, start, y, count, 1)
        for y in (0, Y - 1):
            for z in range(low, high, 2):
                y_flux(z, y, 2, 2)
            y_update(low, y, per, 1)
        for copy in side[2 * chunk:2 * chunk + 2]:
            copy.start()
        if chunk == CHUNKS - 1:
            for z in (0, 1, Z - 2, Z - 1):
                y_update(z, 1, 1, Y - 2)
            for copy in flat + corners:
                copy.start()
    block(y_update, range(2, Z - 2), 1, Y - 2)

    smooth_own(refs2, 2, 1)
    block(planes(refs2, 0, 2), range(2, Z), 1, Y - 2)
    for copy in flat:
        copy.wait()
    ghost_rows(refs2, [(0, 1, 2, Y), (Z + 2, 1, 2, Y)])
    for zs in ((0, 1), (Z, Z + 1)):
        block(planes(refs2, 0, 2), zs, 1, Y - 2)

    def z_flux(z):
        for y in (1, Y // 2):
            face, above = (pl.ds(z, 1), pl.ds(y, 3)), (pl.ds(z + 1, 1), pl.ds(y, 3))
            fz[face] = between(dt, refs2[3:], vz, face, face, above)

    z_flux(0)
    loop(1, Z + 1, z_flux)

    def z_update(z):
        for y in range(1, Y - 1):
            value = (g2[z + 2, y + 1] - fz[z + 1, y] + fz[z, y]) / (
                1.0 - step_value * vz[z + 1, y] + step_value * vz[z, y]
            )
            middle[z, pl.ds(y, T, stride=Y), :] = value

    loop(0, Z, z_update)
    for copy in side + corners:
        copy.wait()
    ghost_rows(refs2, [(0, 0, Z + 4, 1), (0, Y + 1, Z + 4, 1)])
    both(planes(refs2, 0), range(0, Z + 2), (0, Y - 1), 3)


def finish(
    middle, g2, vz, off, ta, tb, sd, step_ref, dt_in, out_hbm, dt_ref, fz, field, sems
):
    Z, T = middle.shape[0], step_ref.shape[0]
    Y = middle.shape[1] // T
    dt_ref[0, 0] = dt_in[0, 0]
    step = step_ref[...]
    dt = step[None, None]
    per = Z // CHUNKS
    copies = []

    def flux(z, count):
        for side, y in enumerate((0, Y - 1)):
            face, above = (pl.ds(z, count), pl.ds(y, 1)), (pl.ds(z + 1, count), pl.ds(y, 1))
            fz[pl.ds(z, count), pl.ds(side, 1)] = between(
                dt, (off, ta, tb, sd), vz, face, face, above
            )

    flux(0, 1)
    for chunk in range(CHUNKS):
        low, high = chunk * per, (chunk + 1) * per
        for z in range(low + 1, high + 1, 2):
            flux(z, 2)
        for z in range(low, high):
            for y in range(1, Y - 1):
                where = pl.ds(y, T, stride=Y)
                field[z, where, :] = middle[z, where, :]
            for side, y in enumerate((0, Y - 1)):
                value = (g2[z + 2, y + 1] - fz[z + 1, side] + fz[z, side]) / (
                    1.0 - step * vz[z + 1, y] + step * vz[z, y]
                )
                field[z, pl.ds(y, T, stride=Y), :] = value
        part = pl.ds(low, per)
        copies.append(pltpu.make_async_copy(field.at[part], out_hbm.at[part], sems.at[chunk]))
        copies[-1].start()
    for copy in copies:
        copy.wait()


def solution(mesh):
    n_gy, n_gz = mesh.shape["gy"], mesh.shape["gz"]

    def shards(*blocks):
        Z, Y, X = blocks[0].shape
        T = X // LANES

        def split(block):
            return block.reshape(Z, Y, T, LANES).transpose(0, 2, 1, 3).reshape(Z, T * Y, LANES)

        def rows(*lead):
            return pltpu.VMEM((*lead, T, LANES), jnp.float32)

        dma = pltpu.SemaphoreType.DMA
        in_vmem = pl.BlockSpec(memory_space=pltpu.VMEM)
        in_smem = pl.BlockSpec(memory_space=pltpu.SMEM)
        kept = (
            pltpu.VMEM((Z, T * Y, LANES), jnp.float32),
            rows(Z + 4, Y + 2), rows(Z + 1, Y), *[rows(Z + 2, Y)] * 4,
        )
        *state, dt = pl.pallas_call(
            functools.partial(kernel, n_gy, n_gz),
            out_shape=(
                *kept, pltpu.VMEM((T, LANES), jnp.float32), pltpu.SMEM((1, 1), jnp.float32),
            ),
            in_specs=[pl.BlockSpec(memory_space=pltpu.HBM)] * 4,
            out_specs=(*[in_vmem] * (len(kept) + 1), in_smem),
            scratch_shapes=[
                *[pltpu.VMEM((Z, T * Y, LANES), jnp.float32)] * 4, dma((4,)),
                rows(Z + 2, Y + 2), rows(Z + 2, Y + 4),
                *[rows(Z + 2, Y + 2)] * 2, *[rows(Z + 2, Y + 4)] * 2, *[rows(Z + 4, Y + 2)] * 2,
                *[rows(Z, Y)] * 4, *[rows(Z, Y + 2)] * 4,
                rows(Z, Y), rows(Z, Y + 1), rows(Z, Y + 1), rows(Z + 1, Y),
                pltpu.VMEM((n_gy * n_gz, 1, LANES), jnp.float32),
                dma((8,)), dma((8,)), *[dma((4 * HALVES + 6,))] * 2, *[dma((2 * CHUNKS + 6,))] * 2,
                dma((2,)), dma((2,)),
                dma((2,)),
            ],
            compiler_params=pltpu.CompilerParams(
                collective_id=0, has_side_effects=True, vmem_limit_bytes=62640128
            ),
        )(*[split(block) for block in blocks])
        field, dt = pl.pallas_call(
            finish,
            out_shape=(
                jax.ShapeDtypeStruct((Z, T * Y, LANES), jnp.float32),
                jax.ShapeDtypeStruct((1, 1), jnp.float32),
            ),
            in_specs=[*[in_vmem] * len(state), in_smem],
            out_specs=(pl.BlockSpec(memory_space=pltpu.HBM), in_smem),
            scratch_shapes=[
                rows(Z + 1, 2), pltpu.VMEM((Z, T * Y, LANES), jnp.float32), dma((CHUNKS,)),
            ],
            compiler_params=pltpu.CompilerParams(vmem_limit_bytes=16777216),
        )(
            *[pltpu.with_memory_space_constraint(value, pltpu.VMEM) for value in state],
            pltpu.with_memory_space_constraint(dt, pltpu.SMEM),
        )
        field = field.reshape(Z, T, Y, LANES).transpose(0, 2, 1, 3).reshape(Z, Y, X)
        return field, dt.reshape(())

    spec = P("gz", "gy", None)
    return jax.shard_map(
        shards, mesh=mesh, in_specs=(spec,) * 4, out_specs=(spec, P()), check_vma=False
    )
```

```python
import functools

import jax
import jax.numpy as jnp
from jax import lax
from jax.experimental import pallas as pl
from jax.experimental.pallas import tpu as pltpu
from jax.sharding import PartitionSpec as P

NEWTON = 5
CHUNKS = 4
HALVES = 2
LANES = 128
GROUP = 8

tilt_floor = 3.2
courant = 0.45
epsilon = 1e-06
tiny = 1e-30
tiny_unit = 1e-15

MESH = pl.DeviceIdType.MESH


def lane_of(value):
    return lax.broadcasted_iota(jnp.int32, value.shape, value.ndim - 1)


def x_next(value):
    turned = pltpu.roll(value, LANES - 1, value.ndim - 1)
    carried = pltpu.roll(turned, value.shape[-2] - 1, value.ndim - 2)
    return jnp.where(lane_of(value) == LANES - 1, carried, turned)


def x_prev(value):
    turned = pltpu.roll(value, 1, value.ndim - 1)
    carried = pltpu.roll(turned, 1, value.ndim - 2)
    return jnp.where(lane_of(value) == 0, carried, turned)


def solve_offset(g, tilt_a, tilt_b, tilt_d):
    volume = jnp.clip(g, 0.0, 1.0)
    lesser = jnp.minimum(volume, 1.0 - volume)
    low = jnp.minimum(tilt_a, tilt_b)
    high = jnp.maximum(tilt_a, tilt_b)
    unit = jnp.maximum(jnp.minimum(low, tilt_d), tiny_unit)
    middle = jnp.maximum(low, tilt_d)
    inverse = 1.0 / unit
    n2 = jnp.minimum(middle, high) * inverse
    n3 = jnp.maximum(middle, high) * inverse
    above = n2 + 1.0
    summed = above + n3
    product = n2 * n3
    target = product * (lesser + lesser)
    gap = 0.5 * jnp.maximum(above - n3, 0.0)
    offset = 0.5 * (summed - (product - target) / (n2 - gap * gap))
    for repeat in range(NEWTON - 1):
        p1 = jnp.minimum(offset, 1.0)
        p2 = jnp.clip(offset - n2, 0.0, 1.0)
        p3 = jnp.maximum(offset - n3, 0.0)
        s1, s2, s3 = p1 * p1, p2 * p2, p3 * p3
        squares = s1 - s2 - s3
        cubes = s1 * p1 - s2 * p2 - s3 * p3
        outer = jnp.clip(offset, 1.0, above)
        q = outer - 1.0
        rate = squares + (q + q)
        offset = (offset * squares - cubes * (1.0 / 3.0) + (q * outer + target)) / rate
    return jnp.where(volume > 0.5, summed - offset, offset) * unit


def face_flux(cross, offset, tilt_a, tilt_b, slope):
    turn = slope * cross
    height = jnp.abs(turn)
    reach = offset - jnp.where(turn > 0, 0.0, jnp.abs(slope) - height)

    def parts(value):
        inside = jnp.maximum(value, 0.0)
        p = jnp.minimum(inside, height)
        q = inside - p
        return p * p * p, q * (q + height)

    reach_a = reach - tilt_a
    p0, q0 = parts(reach)
    p1, q1 = parts(reach_a)
    p2, q2 = parts(reach - tilt_b)
    p3, q3 = parts(reach_a - tilt_b)
    cubes = (p0 - p1) - (p2 - p3)
    wholes = (q0 - q1) - (q2 - q3)
    combo = cubes * ((1.0 / 3.0) / jnp.maximum(height, tiny)) + wholes
    return cross * combo / (2.0 * tilt_a * tilt_b)


def between(dt, planes, velocity, at_face, below, above):
    cross = dt * velocity[at_face]
    upward = cross > 0
    donor = [jnp.where(upward, ref[below], ref[above]) for ref in planes]
    return face_flux(cross, *donor)


def edge_flux(dt, planes, velocity, flux, low, high, y, column):
    while low < high:
        count = min(2, high - low)
        face, above = (pl.ds(low, count), pl.ds(y, 1)), (pl.ds(low + 1, count), pl.ds(y, 1))
        flux[pl.ds(low, count), pl.ds(column, 1)] = between(dt, planes, velocity, face, face, above)
        low += count


def edge_update(g, velocity, flux, field, step, planes, Y, y, column):
    for z in planes:
        value = (g[z + 2, y + 1] - flux[z + 1, column] + flux[z, column]) / (
            1.0 - step * velocity[z + 1, y] + step * velocity[z, y]
        )
        field[z, pl.ds(y, value.shape[0], stride=Y), :] = value


def kernel(
    n_gy, n_gz, f_hbm, vx_hbm, vy_hbm, vz_hbm,
    middle, g2, vz, off2, ta2, tb2, sd2, step_ref,
    f_ref, vx_ref, vy_ref, vz_ref, load_sem,
    g0, g1, sx0, dx0, sx1, dx1, sx2, dx2,
    off0, ta0, tb0, sd0, off1, ta1, tb1, sd1,
    vx, vy, fy, fz, part,
    halo0_send, halo0_recv, halo1_send, halo1_recv, halo2_send, halo2_recv,
    vel_send, vel_recv, part_sem,
):
    Z = f_ref.shape[0]
    T = sx0.shape[2]
    Y = f_ref.shape[1] // T
    loads = []
    for i, (source, target) in enumerate(
        ((f_hbm, f_ref), (vx_hbm, vx_ref), (vy_hbm, vy_ref), (vz_hbm, vz_ref))
    ):
        loads.append(pltpu.make_async_copy(source, target, load_sem.at[i]))
        loads[-1].start()
    my = lax.axis_index("gy")
    mz = lax.axis_index("gz")

    def at(dz, dy):
        return {
            "gy": lax.rem(my + dy + n_gy, n_gy),
            "gz": lax.rem(mz + dz + n_gz, n_gz),
        }

    barrier = pltpu.get_barrier_semaphore()
    def hops(away):
        steps = (away[0] // 2, away[1] // 4, away[1] % 4)
        return sum(min(step, 4 - step) for step in steps)

    greeted = [(a, b) for a in range(n_gz) for b in range(n_gy)][1:]
    greeted.sort(key=hops, reverse=True)
    far = sum(hops(away) >= 4 for away in greeted)
    for dz, dy in greeted:
        pl.semaphore_signal(barrier, inc=1, device_id=at(dz, dy), device_id_type=MESH)

    def rows_of(ref, z, y):
        return ref[z, pl.ds(y, T, stride=Y), :]

    def gather(low, high, body, carry, most=GROUP):
        count = high - low
        grouped = max(u for u in range(1, most + 1) if count % u == 0)

        def step(i, carry):
            for u in range(grouped):
                carry = body(low + i * grouped + u, carry)
            return carry
        return lax.fori_loop(0, count // grouped, step, carry)

    def loop(low, high, body, most=GROUP):
        def step(i, carry):
            body(i)
            return carry
        gather(low, high, step, 0, most)

    def halo_copies(g, spans, sends, recvs):
        copies = []
        for index, (dz, dy, src_z, dst_z, src_y, dst_y) in enumerate(spans):
            copies.append(pltpu.make_async_remote_copy(
                src_ref=g.at[src_z, src_y],
                dst_ref=g.at[dst_z, dst_y],
                send_sem=sends.at[index],
                recv_sem=recvs.at[index],
                device_id=at(dz, dy),
                device_id_type=MESH,
            ))
        return copies

    def span(side, count, pad, depth):
        if side == 0:
            return pl.ds(pad, count), pl.ds(pad, count)
        if side > 0:
            return pl.ds(pad + count - depth, depth), pl.ds(pad - depth, depth)
        return pl.ds(pad, depth), pl.ds(pad + count, depth)

    def spans_for(sides, pad_z, pad_y):
        return [
            (dz, dy, *span(dz, Z, pad_z, pad_z), *span(dy, Y, pad_y, pad_y))
            for dz, dy in sides
        ]

    Y_SIDES = [(0, -1), (0, 1)]
    Z_SIDES = [(-1, 0), (1, 0)]
    CORNERS = [(a, b) for a in (-1, 1) for b in (-1, 1)]

    def smooth_rows(g, sx, dx, z, y, kz, ky):
        value = g[pl.ds(z, kz), pl.ds(y, ky)]
        after, before = x_next(value), x_prev(value)
        sx[pl.ds(z, kz), pl.ds(y, ky)] = before + (value + value) + after
        dx[pl.ds(z, kz), pl.ds(y, ky)] = after - before

    def smooth_zero(arr):
        mid = arr[1:-1]
        return (arr[:-2] + mid) + (mid + arr[2:])

    def smooth_one(arr):
        pair = arr[:, :-1] + arr[:, 1:]
        return pair[:, :-1] + pair[:, 1:]

    def plane(refs, dim, z, y, kz, ky, parts=1):
        g, sx, dx, off, ta, tb, sd = refs
        s = sx[pl.ds(z, kz + 2), pl.ds(y, ky + 2)]
        d = dx[pl.ds(z, kz + 2), pl.ds(y, ky + 2)]
        grad_zero = smooth_one(s[2:] - s[:-2])
        across = smooth_zero(s)
        grad_one = (across[:, 2:] - across[:, :-2])
        grad_cells = smooth_one(smooth_zero(d))
        slopes = (grad_zero, grad_one, grad_cells)
        low = 0
        for part in range(parts):
            count = (ky - low) // (parts - part)
            cut = [value[:, low:low + count] for value in slopes]
            slope = cut[dim]
            tilt_a, tilt_b = [jnp.abs(cut[e]) + tilt_floor for e in range(3) if e != dim]
            value = g[pl.ds(z + 1, kz), pl.ds(y + 1 + low, count)]
            where = (pl.ds(z, kz), pl.ds(y + low, count))
            off[where] = solve_offset(value, tilt_a, tilt_b, jnp.abs(slope))
            ta[where] = tilt_a
            tb[where] = tilt_b
            sd[where] = slope
            low += count

    def block(body, zs, y, ky, kz=1):
        count = len(zs) // kz
        step = zs[1] - zs[0] if len(zs) > 1 else 1
        loop(0, count, lambda i: body(zs[0] + step * kz * i, y, kz, ky))

    def both(body, zs, ys, kz=2):
        count = len(zs) // kz

        def step(i):
            for y in ys:
                body(zs[0] + kz * i, y, kz, 1)
        loop(0, count, step)

    def planes(refs, dim, parts=1):
        return lambda z, y, kz, ky: plane(refs, dim, z, y, kz, ky, parts)

    def smooth_own(refs, z, y):
        loop(z, z + Z, lambda i: smooth_rows(*refs[:3], i, y, 1, Y), Z)

    own = range(0, Z)
    refs0 = (g0, sx0, dx0, off0, ta0, tb0, sd0)
    refs1 = (g1, sx1, dx1, off1, ta1, tb1, sd1)
    refs2 = (g2, sx2, dx2, off2, ta2, tb2, sd2)

    def donors(z, y, kz, ky):
        where = (pl.ds(z, kz), pl.ds(y, ky))
        upward = vx[where] > 0
        for ref in (off0, ta0, tb0, sd0):
            value = ref[where]
            ref[where] = jnp.where(upward, value, x_next(value))

    def donors_in():
        loop(1, Z - 1, lambda z: donors(z, 1, 1, Y - 2))

    def ghost_rows(refs, spans):
        for z, y, kz, ky in spans:
            smooth_rows(*refs[:3], z, y, kz, ky)

    def fill(z, total):
        for y in range(Y):
            f = rows_of(f_ref, z, y)
            g0[z + 1, y + 1] = f
            total = total + 4.0 * f * (1.0 - f)
        return total

    loads[0].wait()
    total = gather(0, Z, fill, jnp.zeros((T, LANES), jnp.float32))

    def fill_velocity(z, peak):
        for y in range(Y):
            a = rows_of(vx_ref, z, y)
            b = rows_of(vy_ref, z, y)
            c = rows_of(vz_ref, z, y)
            vx[z, y] = a
            vy[z, y + 1] = b
            vz[z + 1, y] = c
            peak = jnp.maximum(peak, jnp.maximum(jnp.abs(a), jnp.maximum(jnp.abs(b), jnp.abs(c))))
        return peak

    for copy in loads[1:]:
        copy.wait()
    peak = gather(0, Z, fill_velocity, jnp.zeros((T, LANES), jnp.float32))
    low_lanes = lane_of(jnp.zeros((1, LANES), jnp.float32)) < LANES // 2

    def folded(sums, peaks):
        sums = jnp.sum(sums, axis=0, keepdims=True)
        peaks = jnp.max(peaks, axis=0, keepdims=True)
        sums = sums + pltpu.roll(sums, LANES // 2, 1)
        peaks = jnp.maximum(peaks, pltpu.roll(peaks, LANES // 2, 1))
        return jnp.where(low_lanes, sums, peaks)

    me = mz * n_gy + my
    part[me] = folded(total, peak)
    pl.semaphore_wait(barrier, len(greeted))
    vel_copies = [
        pltpu.make_async_remote_copy(
            src_ref=vy.at[:, pl.ds(Y, 1)], dst_ref=vy.at[:, pl.ds(0, 1)],
            send_sem=vel_send.at[0], recv_sem=vel_recv.at[0],
            device_id=at(0, 1), device_id_type=MESH,
        ),
        pltpu.make_async_remote_copy(
            src_ref=vz.at[pl.ds(Z, 1)], dst_ref=vz.at[pl.ds(0, 1)],
            send_sem=vel_send.at[1], recv_sem=vel_recv.at[1],
            device_id=at(1, 0), device_id_type=MESH,
        ),
    ]

    halos0 = halo_copies(
        g0, spans_for(Y_SIDES + Z_SIDES + CORNERS, 1, 1), halo0_send, halo0_recv
    )
    part_copies = [
        pltpu.make_async_remote_copy(
            src_ref=part.at[me], dst_ref=part.at[me],
            send_sem=part_sem.at[0], recv_sem=part_sem.at[1],
            device_id=at(*away), device_id_type=MESH,
        )
        for away in greeted
    ]
    for copy in part_copies[:far] + halos0 + part_copies[far:]:
        copy.start()

    smooth_own(refs0, 1, 1)
    block(planes(refs0, 2, 2), range(1, Z - 1), 1, Y - 2)
    donors_in()
    for copy in vel_copies:
        copy.start()
    for copy in halos0[2:4]:
        copy.wait()
    ghost_rows(refs0, [(0, 1, 1, Y), (Z + 1, 1, 1, Y)])
    block(planes(refs0, 2, 2), (0, Z - 1), 1, Y - 2)
    for z in (0, Z - 1):
        donors(z, 1, 1, Y - 2)
    for copy in halos0[:2] + halos0[4:]:
        copy.wait()
    ghost_rows(refs0, [(0, 0, Z + 2, 1), (0, Y + 1, Z + 2, 1)])
    both(planes(refs0, 2), own, (0, Y - 1))
    both(donors, own, (0, Y - 1), 4)
    others = pl.ds(0, len(greeted))
    arrived = pltpu.make_async_remote_copy(
        src_ref=part.at[others], dst_ref=part.at[others],
        send_sem=part_sem.at[0], recv_sem=part_sem.at[1],
        device_id=at(*greeted[0]), device_id_type=MESH,
    )
    arrived.wait()
    sums = peaks = part[0]
    for i in range(1, n_gy * n_gz):
        sums = sums + part[i]
        peaks = jnp.maximum(peaks, part[i])
    sums = jnp.where(low_lanes, sums, 0.0)
    peaks = jnp.where(low_lanes, 0.0, peaks)
    cells_all = float(Z * Y * T * LANES * n_gy * n_gz)
    share = jnp.broadcast_to(jnp.sum(sums, keepdims=True), (T, LANES)) / cells_all
    umax = jnp.broadcast_to(jnp.max(peaks, keepdims=True), (T, LANES))
    step_value = courant / ((umax + epsilon) * (1.0 + share))
    step_ref[...] = step_value
    dt = step_value[None, None]

    def x_update(z, y, kz, ky):
        where = (pl.ds(z, kz), pl.ds(y, ky))
        cross = dt * vx[where]
        flux = face_flux(cross, off0[where], ta0[where], tb0[where], sd0[where])
        value = g0[pl.ds(z + 1, kz), pl.ds(y + 1, ky)]
        g1[pl.ds(z + 1, kz), pl.ds(y + 2, ky)] = (value - flux + x_prev(flux)) / (
            1.0 - cross + x_prev(cross)
        )

    def y_flux(z, y, kz, ky):
        rows = pl.ds(z, kz)
        face = (rows, pl.ds(y, ky))
        fy[face] = between(dt, refs1[3:], vy, face, face, (rows, pl.ds(y + 1, ky)))

    def y_update(z, y, kz, ky):
        rows = pl.ds(z, kz)
        low, high = pl.ds(y, ky), pl.ds(y + 1, ky)
        value = g1[pl.ds(z + 1, kz), pl.ds(y + 2, ky)]
        g2[pl.ds(z + 2, kz), pl.ds(y + 1, ky)] = (value - fy[rows, high] + fy[rows, low]) / (
            1.0 - dt * vy[rows, high] + dt * vy[rows, low]
        )

    middle_row = Z // 2 + 1
    halves = ((0, middle_row), (middle_row, Z))
    spans1 = []
    for depth in (1, 2):
        for low, high in halves:
            for dy in (-1, 1):
                src, dst = span(dy, Y, 2, 2)
                near = (0, 1)[(dy > 0) == (depth == 1)]
                rows = pl.ds(1 + low, high - low)
                spans1.append((
                    0, dy, rows, rows,
                    pl.ds(src.start + near, 1), pl.ds(dst.start + near, 1),
                ))
    deep = len(spans1)
    for dz in (-1, 1):
        spans1.append((dz, 0, *span(dz, Z, 1, 1), pl.ds(2, Y), pl.ds(2, Y)))
    spans1 += spans_for(CORNERS, 1, 2)
    halos1 = halo_copies(g1, spans1, halo1_send, halo1_recv)
    first = halos1[:deep // 2]
    second = halos1[deep // 2:deep]
    flat1, corners1 = halos1[deep:deep + 2], halos1[deep + 2:]

    for copies, ys in ((first, (0, Y - 1)), (second, (1, Y - 2))):
        for at_half, (low, high) in enumerate(halves):
            both(x_update, range(low, high), ys, 3 if (high - low) % 3 == 0 else 1)
            for copy in copies[2 * at_half:2 * at_half + 2]:
                copy.start()
    block(x_update, (0, Z - 1), 2, Y - 4)
    for copy in flat1 + corners1:
        copy.start()
    block(x_update, range(1, Z - 1), 2, Y - 4)
    smooth_own(refs1, 1, 2)
    block(planes(refs1, 1, 2), range(1, Z - 1), 2, Y - 2)
    for copy in flat1:
        copy.wait()
    ghost_rows(refs1, [(0, 2, 1, Y), (Z + 1, 2, 1, Y)])
    block(planes(refs1, 1, 2), (0, Z - 1), 2, Y - 2)
    block(y_flux, own, 2, 2)
    block(y_flux, own, 4, Y - 5)
    for copy in vel_copies:
        copy.wait()
    for at_half, (low, high) in enumerate(halves):
        for copy in first[2 * at_half:2 * at_half + 2]:
            copy.wait()
        ghost_rows(refs1, [(1 + low, y, high - low, 1) for y in (1, Y + 2)])
        both(planes(refs1, 1), range(max(low - 1, 1), high - 1), (1, Y), 1)

    per = Z // CHUNKS
    spans2 = []
    for low in range(0, Z, per):
        for dy in (-1, 1):
            rows = pl.ds(2 + low, per)
            spans2.append((0, dy, rows, rows, *span(dy, Y, 1, 1)))
    spans2 += spans_for(Z_SIDES + CORNERS, 2, 1)
    halos2 = halo_copies(g2, spans2, halo2_send, halo2_recv)
    side, flat, corners = halos2[:2 * CHUNKS], halos2[2 * CHUNKS:-4], halos2[-4:]

    def chunk_out(chunk):
        low, high = chunk * per, (chunk + 1) * per
        start, count = max(low, 1), min(high, Z - 1) - max(low, 1)
        for y in (0, Y + 1):
            plane(refs1, 1, start, y, count, 1)
        for y in (0, Y - 1):
            for z in range(low, high, 2):
                y_flux(z, y, 2, 2)
            y_update(low, y, per, 1)
        for copy in side[2 * chunk:2 * chunk + 2]:
            copy.start()

    for at_half, (low, high) in enumerate(halves):
        for copy in second[2 * at_half:2 * at_half + 2] + corners1[2 - 2 * at_half:4 - 2 * at_half]:
            copy.wait()
        end = at_half * (Z - 1)
        ghost = at_half * (Z + 1)
        ghost_rows(refs1, [(1 + low, y, high - low, 1) for y in (0, Y + 3)])
        ghost_rows(refs1, [(ghost, 0, 1, 2), (ghost, Y + 2, 1, 2)])
        for y in (0, Y):
            plane(refs1, 1, end, y, 1, 2)
        chunk_out(at_half * (CHUNKS - 1))
        for z in (end, end + 1 - 2 * at_half):
            y_update(z, 1, 1, Y - 2)
        for copy in [flat[at_half]] + corners[2 * at_half:2 * at_half + 2]:
            copy.start()
        chunk_out(1 + at_half)
    block(y_update, range(2, Z - 2), 1, Y - 2)

    smooth_own(refs2, 2, 1)
    block(planes(refs2, 0, 2), range(2, Z), 1, Y - 2)
    for copy in flat:
        copy.wait()
    ghost_rows(refs2, [(0, 1, 2, Y), (Z + 2, 1, 2, Y)])
    for zs in ((0, 1), (Z, Z + 1)):
        block(planes(refs2, 0, 2), zs, 1, Y - 2)

    def z_flux(z):
        for y in (1, Y // 2):
            face, above = (pl.ds(z, 1), pl.ds(y, 3)), (pl.ds(z + 1, 1), pl.ds(y, 3))
            fz[face] = between(dt, refs2[3:], vz, face, face, above)

    z_flux(0)
    loop(1, Z + 1, z_flux)

    def z_update(z):
        for y in range(1, Y - 1):
            value = (g2[z + 2, y + 1] - fz[z + 1, y] + fz[z, y]) / (
                1.0 - step_value * vz[z + 1, y] + step_value * vz[z, y]
            )
            middle[z, pl.ds(y, T, stride=Y), :] = value

    loop(0, Z, z_update)
    for copy in side[:4] + corners[2:]:
        copy.wait()
    first_rows = 2 + Z // 2
    ghost_rows(refs2, [(0, y, first_rows, 1) for y in (0, Y + 1)])
    both(planes(refs2, 0), range(0, first_rows - 2), (0, Y - 1))
    for y in (0, Y - 1):
        edge_flux(dt, refs2[3:], vz, fz, 0, per + 1, y, y)
        edge_update(g2, vz, fz, middle, step_value, range(0, per), Y, y, y)
    for copy in side[4:] + corners[:2]:
        copy.wait()
    ghost_rows(refs2, [(first_rows, y, Z + 4 - first_rows, 1) for y in (0, Y + 1)])
    both(planes(refs2, 0), range(first_rows - 2, Z + 2), (0, Y - 1))


def finish(
    middle, g2, vz, off, ta, tb, sd, step_ref, out_hbm, dt_hbm, fz, field, one, sems
):
    Z, T = middle.shape[0], step_ref.shape[0]
    Y = middle.shape[1] // T
    step = step_ref[...]
    one[...] = step[:1, :1]
    copies = [pltpu.make_async_copy(one, dt_hbm, sems.at[CHUNKS])]
    copies[0].start()
    dt = step[None, None]
    per = Z // CHUNKS
    for chunk in range(CHUNKS):
        low, high = chunk * per, (chunk + 1) * per
        if chunk > 0:
            for side, y in enumerate((0, Y - 1)):
                new = low if chunk == 1 else low + 1
                edge_flux(dt, (off, ta, tb, sd), vz, fz, new, high + 1, y, side)
                edge_update(g2, vz, fz, field, step, range(low, high), Y, y, side)
            for z in range(low, high):
                for y in range(1, Y - 1):
                    where = pl.ds(y, T, stride=Y)
                    field[z, where, :] = middle[z, where, :]
        part = pl.ds(low, per)
        source = field if chunk > 0 else middle
        copies.append(pltpu.make_async_copy(source.at[part], out_hbm.at[part], sems.at[chunk]))
        copies[-1].start()
    for copy in copies:
        copy.wait()


def solution(mesh):
    n_gy, n_gz = mesh.shape["gy"], mesh.shape["gz"]

    def shards(*blocks):
        Z, Y, X = blocks[0].shape
        T = X // LANES

        def split(block):
            return block.reshape(Z, Y, T, LANES).transpose(0, 2, 1, 3).reshape(Z, T * Y, LANES)

        def rows(*lead):
            return pltpu.VMEM((*lead, T, LANES), jnp.float32)

        dma = pltpu.SemaphoreType.DMA
        in_vmem = pl.BlockSpec(memory_space=pltpu.VMEM)
        kept = (
            pltpu.VMEM((Z, T * Y, LANES), jnp.float32),
            rows(Z + 4, Y + 2), rows(Z + 1, Y), *[rows(Z + 2, Y)] * 4,
        )
        state = pl.pallas_call(
            functools.partial(kernel, n_gy, n_gz),
            out_shape=(
                *kept, pltpu.VMEM((T, LANES), jnp.float32),
            ),
            in_specs=[pl.BlockSpec(memory_space=pltpu.HBM)] * 4,
            out_specs=(in_vmem,) * (len(kept) + 1),
            scratch_shapes=[
                *[pltpu.VMEM((Z, T * Y, LANES), jnp.float32)] * 4, dma((4,)),
                rows(Z + 2, Y + 2), rows(Z + 2, Y + 4),
                *[rows(Z + 2, Y + 2)] * 2, *[rows(Z + 2, Y + 4)] * 2, *[rows(Z + 4, Y + 2)] * 2,
                *[rows(Z, Y)] * 4, *[rows(Z, Y + 2)] * 4,
                rows(Z, Y), rows(Z, Y + 1), rows(Z, Y + 1), rows(Z + 1, Y),
                pltpu.VMEM((n_gy * n_gz, 1, LANES), jnp.float32),
                dma((8,)), dma((8,)), *[dma((4 * HALVES + 6,))] * 2, *[dma((2 * CHUNKS + 6,))] * 2,
                dma((2,)), dma((2,)),
                dma((2,)),
            ],
            compiler_params=pltpu.CompilerParams(
                collective_id=0, has_side_effects=True, vmem_limit_bytes=62640128
            ),
        )(*[split(block) for block in blocks])
        field, dt = pl.pallas_call(
            finish,
            out_shape=(
                jax.ShapeDtypeStruct((Z, T * Y, LANES), jnp.float32),
                jax.ShapeDtypeStruct((1, 1), jnp.float32),
            ),
            in_specs=[in_vmem] * len(state),
            out_specs=(pl.BlockSpec(memory_space=pltpu.HBM),) * 2,
            scratch_shapes=[
                rows(Z + 1, 2), pltpu.VMEM((Z, T * Y, LANES), jnp.float32),
                pltpu.VMEM((1, 1), jnp.float32), dma((CHUNKS + 1,)),
            ],
            compiler_params=pltpu.CompilerParams(vmem_limit_bytes=16777216),
        )(
            *[pltpu.with_memory_space_constraint(value, pltpu.VMEM) for value in state],
        )
        field = field.reshape(Z, T, Y, LANES).transpose(0, 2, 1, 3).reshape(Z, Y, X)
        return field, dt.reshape(())

    spec = P("gz", "gy", None)
    return jax.shard_map(
        shards, mesh=mesh, in_specs=(spec,) * 4, out_specs=(spec, P()), check_vma=False
    )
```

```python
import functools

import jax
import jax.numpy as jnp
from jax import lax
from jax.experimental import pallas as pl
from jax.experimental.pallas import tpu as pltpu
from jax.sharding import PartitionSpec as P

NEWTON = 5
CHUNKS = 4
HALVES = 2
LANES = 128
GROUP = 8

tilt_floor = 3.2
courant = 0.45
epsilon = 1e-06
tiny = 1e-30
tiny_unit = 1e-15

MESH = pl.DeviceIdType.MESH


def lane_of(value):
    return lax.broadcasted_iota(jnp.int32, value.shape, value.ndim - 1)


def x_next(value):
    turned = pltpu.roll(value, LANES - 1, value.ndim - 1)
    carried = pltpu.roll(turned, value.shape[-2] - 1, value.ndim - 2)
    return jnp.where(lane_of(value) == LANES - 1, carried, turned)


def x_prev(value):
    turned = pltpu.roll(value, 1, value.ndim - 1)
    carried = pltpu.roll(turned, 1, value.ndim - 2)
    return jnp.where(lane_of(value) == 0, carried, turned)


def solve_offset(g, tilt_a, tilt_b, tilt_d):
    volume = jnp.clip(g, 0.0, 1.0)
    lesser = jnp.minimum(volume, 1.0 - volume)
    low = jnp.minimum(tilt_a, tilt_b)
    high = jnp.maximum(tilt_a, tilt_b)
    unit = jnp.maximum(jnp.minimum(low, tilt_d), tiny_unit)
    middle = jnp.maximum(low, tilt_d)
    inverse = 1.0 / unit
    n2 = jnp.minimum(middle, high) * inverse
    n3 = jnp.maximum(middle, high) * inverse
    above = n2 + 1.0
    summed = above + n3
    product = n2 * n3
    target = product * (lesser + lesser)
    gap = 0.5 * jnp.maximum(above - n3, 0.0)
    offset = 0.5 * (summed - (product - target) / (n2 - gap * gap))
    for repeat in range(NEWTON - 1):
        p1 = jnp.minimum(offset, 1.0)
        p2 = jnp.clip(offset - n2, 0.0, 1.0)
        p3 = jnp.maximum(offset - n3, 0.0)
        s1, s2, s3 = p1 * p1, p2 * p2, p3 * p3
        squares = s1 - s2 - s3
        cubes = s1 * p1 - s2 * p2 - s3 * p3
        outer = jnp.clip(offset, 1.0, above)
        q = outer - 1.0
        rate = squares + (q + q)
        offset = (offset * squares - cubes * (1.0 / 3.0) + (q * outer + target)) / rate
    return jnp.where(volume > 0.5, summed - offset, offset) * unit


def face_flux(cross, offset, tilt_a, tilt_b, slope):
    turn = slope * cross
    height = jnp.abs(turn)
    reach = offset - jnp.where(turn > 0, 0.0, jnp.abs(slope) - height)

    def parts(value):
        inside = jnp.maximum(value, 0.0)
        p = jnp.minimum(inside, height)
        q = inside - p
        return p * p * p, q * (q + height)

    reach_a = reach - tilt_a
    p0, q0 = parts(reach)
    p1, q1 = parts(reach_a)
    p2, q2 = parts(reach - tilt_b)
    p3, q3 = parts(reach_a - tilt_b)
    cubes = (p0 - p1) - (p2 - p3)
    wholes = (q0 - q1) - (q2 - q3)
    combo = cubes * ((1.0 / 3.0) / jnp.maximum(height, tiny)) + wholes
    return cross * combo / (2.0 * tilt_a * tilt_b)


def between(dt, planes, velocity, at_face, below, above):
    cross = dt * velocity[at_face]
    upward = cross > 0
    donor = [jnp.where(upward, ref[below], ref[above]) for ref in planes]
    return face_flux(cross, *donor)


def edge_flux(dt, planes, velocity, flux, low, high, y, column):
    while low < high:
        count = min(2, high - low)
        face, above = (pl.ds(low, count), pl.ds(y, 1)), (pl.ds(low + 1, count), pl.ds(y, 1))
        flux[pl.ds(low, count), pl.ds(column, 1)] = between(dt, planes, velocity, face, face, above)
        low += count


def edge_update(g, velocity, flux, field, step, planes, Y, y, column):
    for z in planes:
        value = (g[z + 2, y + 1] - flux[z + 1, column] + flux[z, column]) / (
            1.0 - step * velocity[z + 1, y] + step * velocity[z, y]
        )
        field[z, pl.ds(y, value.shape[0], stride=Y), :] = value


def kernel(
    n_gy, n_gz, f_hbm, vx_hbm, vy_hbm, vz_hbm,
    middle, g2, vz, off2, ta2, tb2, sd2, step_ref,
    f_ref, vx_ref, vy_ref, vz_ref, load_sem,
    g0, g1, sx0, dx0, sx1, dx1, sx2, dx2,
    off0, ta0, tb0, sd0, off1, ta1, tb1, sd1,
    vx, vy, fy, fz, part,
    halo0_send, halo0_recv, halo1_send, halo1_recv, halo2_send, halo2_recv,
    vel_send, vel_recv, part_sem,
):
    Z = f_ref.shape[0]
    T = sx0.shape[2]
    Y = f_ref.shape[1] // T
    loads = []
    for i, (source, target) in enumerate(
        ((f_hbm, f_ref), (vx_hbm, vx_ref), (vy_hbm, vy_ref), (vz_hbm, vz_ref))
    ):
        loads.append(pltpu.make_async_copy(source, target, load_sem.at[i]))
        loads[-1].start()
    my = lax.axis_index("gy")
    mz = lax.axis_index("gz")

    def at(dz, dy):
        return {
            "gy": lax.rem(my + dy + n_gy, n_gy),
            "gz": lax.rem(mz + dz + n_gz, n_gz),
        }

    barrier = pltpu.get_barrier_semaphore()
    def hops(away):
        steps = (away[0] // 2, away[1] // 4, away[1] % 4)
        return sum(min(step, 4 - step) for step in steps)

    greeted = [(a, b) for a in range(n_gz) for b in range(n_gy)][1:]
    greeted.sort(key=hops, reverse=True)
    far = sum(hops(away) >= 4 for away in greeted)
    for dz, dy in greeted:
        pl.semaphore_signal(barrier, inc=1, device_id=at(dz, dy), device_id_type=MESH)

    def rows_of(ref, z, y):
        return ref[z, pl.ds(y, T, stride=Y), :]

    def gather(low, high, body, carry, most=GROUP):
        count = high - low
        grouped = max(u for u in range(1, most + 1) if count % u == 0)

        def step(i, carry):
            for u in range(grouped):
                carry = body(low + i * grouped + u, carry)
            return carry
        return lax.fori_loop(0, count // grouped, step, carry)

    def loop(low, high, body, most=GROUP):
        def step(i, carry):
            body(i)
            return carry
        gather(low, high, step, 0, most)

    def halo_copies(g, spans, sends, recvs):
        copies = []
        for index, (dz, dy, src_z, dst_z, src_y, dst_y) in enumerate(spans):
            copies.append(pltpu.make_async_remote_copy(
                src_ref=g.at[src_z, src_y],
                dst_ref=g.at[dst_z, dst_y],
                send_sem=sends.at[index],
                recv_sem=recvs.at[index],
                device_id=at(dz, dy),
                device_id_type=MESH,
            ))
        return copies

    def span(side, count, pad, depth):
        if side == 0:
            return pl.ds(pad, count), pl.ds(pad, count)
        if side > 0:
            return pl.ds(pad + count - depth, depth), pl.ds(pad - depth, depth)
        return pl.ds(pad, depth), pl.ds(pad + count, depth)

    def spans_for(sides, pad_z, pad_y):
        return [
            (dz, dy, *span(dz, Z, pad_z, pad_z), *span(dy, Y, pad_y, pad_y))
            for dz, dy in sides
        ]

    Y_SIDES = [(0, -1), (0, 1)]
    Z_SIDES = [(-1, 0), (1, 0)]
    CORNERS = [(a, b) for a in (-1, 1) for b in (-1, 1)]

    def smooth_rows(g, sx, dx, z, y, kz, ky):
        value = g[pl.ds(z, kz), pl.ds(y, ky)]
        after, before = x_next(value), x_prev(value)
        sx[pl.ds(z, kz), pl.ds(y, ky)] = before + (value + value) + after
        dx[pl.ds(z, kz), pl.ds(y, ky)] = after - before

    def smooth_zero(arr):
        mid = arr[1:-1]
        return (arr[:-2] + mid) + (mid + arr[2:])

    def smooth_one(arr):
        pair = arr[:, :-1] + arr[:, 1:]
        return pair[:, :-1] + pair[:, 1:]

    def plane(refs, dim, z, y, kz, ky, parts=1):
        g, sx, dx, off, ta, tb, sd = refs
        s = sx[pl.ds(z, kz + 2), pl.ds(y, ky + 2)]
        d = dx[pl.ds(z, kz + 2), pl.ds(y, ky + 2)]
        grad_zero = smooth_one(s[2:] - s[:-2])
        across = smooth_zero(s)
        grad_one = (across[:, 2:] - across[:, :-2])
        grad_cells = smooth_one(smooth_zero(d))
        slopes = (grad_zero, grad_one, grad_cells)
        low = 0
        for part in range(parts):
            count = (ky - low) // (parts - part)
            cut = [value[:, low:low + count] for value in slopes]
            slope = cut[dim]
            tilt_a, tilt_b = [jnp.abs(cut[e]) + tilt_floor for e in range(3) if e != dim]
            value = g[pl.ds(z + 1, kz), pl.ds(y + 1 + low, count)]
            where = (pl.ds(z, kz), pl.ds(y + low, count))
            off[where] = solve_offset(value, tilt_a, tilt_b, jnp.abs(slope))
            ta[where] = tilt_a
            tb[where] = tilt_b
            sd[where] = slope
            low += count

    def block(body, zs, y, ky, kz=1):
        count = len(zs) // kz
        step = zs[1] - zs[0] if len(zs) > 1 else 1
        loop(0, count, lambda i: body(zs[0] + step * kz * i, y, kz, ky))

    def both(body, zs, ys, kz=2):
        count = len(zs) // kz

        def step(i):
            for y in ys:
                body(zs[0] + kz * i, y, kz, 1)
        loop(0, count, step)

    def planes(refs, dim, parts=1):
        return lambda z, y, kz, ky: plane(refs, dim, z, y, kz, ky, parts)

    def smooth_own(refs, z, y):
        loop(z, z + Z, lambda i: smooth_rows(*refs[:3], i, y, 1, Y), Z)

    own = range(0, Z)
    refs0 = (g0, sx0, dx0, off0, ta0, tb0, sd0)
    refs1 = (g1, sx1, dx1, off1, ta1, tb1, sd1)
    refs2 = (g2, sx2, dx2, off2, ta2, tb2, sd2)

    def donors(z, y, kz, ky):
        where = (pl.ds(z, kz), pl.ds(y, ky))
        upward = vx[where] > 0
        for ref in (off0, ta0, tb0, sd0):
            value = ref[where]
            ref[where] = jnp.where(upward, value, x_next(value))

    def donors_in():
        loop(1, Z - 1, lambda z: donors(z, 1, 1, Y - 2))

    def ghost_rows(refs, spans):
        for z, y, kz, ky in spans:
            smooth_rows(*refs[:3], z, y, kz, ky)

    def fill(z, total):
        for y in range(Y):
            f = rows_of(f_ref, z, y)
            g0[z + 1, y + 1] = f
            total = total + 4.0 * f * (1.0 - f)
        return total

    loads[0].wait()
    total = gather(0, Z, fill, jnp.zeros((T, LANES), jnp.float32))

    def fill_velocity(z, peak):
        for y in range(Y):
            a = rows_of(vx_ref, z, y)
            b = rows_of(vy_ref, z, y)
            c = rows_of(vz_ref, z, y)
            vx[z, y] = a
            vy[z, y + 1] = b
            vz[z + 1, y] = c
            peak = jnp.maximum(peak, jnp.maximum(jnp.abs(a), jnp.maximum(jnp.abs(b), jnp.abs(c))))
        return peak

    for copy in loads[1:]:
        copy.wait()
    peak = gather(0, Z, fill_velocity, jnp.zeros((T, LANES), jnp.float32))
    low_lanes = lane_of(jnp.zeros((1, LANES), jnp.float32)) < LANES // 2

    def folded(sums, peaks):
        sums = jnp.sum(sums, axis=0, keepdims=True)
        peaks = jnp.max(peaks, axis=0, keepdims=True)
        sums = sums + pltpu.roll(sums, LANES // 2, 1)
        peaks = jnp.maximum(peaks, pltpu.roll(peaks, LANES // 2, 1))
        return jnp.where(low_lanes, sums, peaks)

    me = mz * n_gy + my
    part[me] = folded(total, peak)
    pl.semaphore_wait(barrier, len(greeted))
    vel_copies = [
        pltpu.make_async_remote_copy(
            src_ref=vy.at[:, pl.ds(Y, 1)], dst_ref=vy.at[:, pl.ds(0, 1)],
            send_sem=vel_send.at[0], recv_sem=vel_recv.at[0],
            device_id=at(0, 1), device_id_type=MESH,
        ),
        pltpu.make_async_remote_copy(
            src_ref=vz.at[pl.ds(Z, 1)], dst_ref=vz.at[pl.ds(0, 1)],
            send_sem=vel_send.at[1], recv_sem=vel_recv.at[1],
            device_id=at(1, 0), device_id_type=MESH,
        ),
    ]

    halos0 = halo_copies(
        g0, spans_for(Y_SIDES + Z_SIDES + CORNERS, 1, 1), halo0_send, halo0_recv
    )
    part_copies = [
        pltpu.make_async_remote_copy(
            src_ref=part.at[me], dst_ref=part.at[me],
            send_sem=part_sem.at[0], recv_sem=part_sem.at[1],
            device_id=at(*away), device_id_type=MESH,
        )
        for away in greeted
    ]
    for copy in halos0[4:] + halos0[2:4] + part_copies[:far] + halos0[:2] + part_copies[far:]:
        copy.start()

    smooth_own(refs0, 1, 1)
    block(planes(refs0, 2, 2), range(1, Z - 1), 1, Y - 2)
    donors_in()
    for copy in vel_copies:
        copy.start()
    for copy in halos0[2:4]:
        copy.wait()
    ghost_rows(refs0, [(0, 1, 1, Y), (Z + 1, 1, 1, Y)])
    block(planes(refs0, 2, 2), (0, Z - 1), 1, Y - 2)
    for z in (0, Z - 1):
        donors(z, 1, 1, Y - 2)
    for copy in halos0[:2] + halos0[4:]:
        copy.wait()
    ghost_rows(refs0, [(0, 0, Z + 2, 1), (0, Y + 1, Z + 2, 1)])
    both(planes(refs0, 2), own, (0, Y - 1))
    both(donors, own, (0, Y - 1), 4)
    others = pl.ds(0, len(greeted))
    arrived = pltpu.make_async_remote_copy(
        src_ref=part.at[others], dst_ref=part.at[others],
        send_sem=part_sem.at[0], recv_sem=part_sem.at[1],
        device_id=at(*greeted[0]), device_id_type=MESH,
    )
    arrived.wait()
    sums = [part[i] for i in range(GROUP)]
    peaks = list(sums)
    for i in range(len(sums), n_gy * n_gz):
        at_row = i % len(sums)
        row = part[i]
        sums[at_row] = sums[at_row] + row
        peaks[at_row] = jnp.maximum(peaks[at_row], row)
    while len(sums) > 1:
        count = len(sums) // 2
        sums = [sums[i] + sums[i + count] for i in range(count)]
        peaks = [jnp.maximum(peaks[i], peaks[i + count]) for i in range(count)]
    sums, peaks = sums[0], peaks[0]
    sums = jnp.where(low_lanes, sums, 0.0)
    peaks = jnp.where(low_lanes, 0.0, peaks)
    cells_all = float(Z * Y * T * LANES * n_gy * n_gz)
    share = jnp.broadcast_to(jnp.sum(sums, keepdims=True), (T, LANES)) / cells_all
    umax = jnp.broadcast_to(jnp.max(peaks, keepdims=True), (T, LANES))
    step_value = courant / ((umax + epsilon) * (1.0 + share))
    step_ref[...] = step_value
    dt = step_value[None, None]

    def x_update(z, y, kz, ky):
        where = (pl.ds(z, kz), pl.ds(y, ky))
        cross = dt * vx[where]
        flux = face_flux(cross, off0[where], ta0[where], tb0[where], sd0[where])
        value = g0[pl.ds(z + 1, kz), pl.ds(y + 1, ky)]
        g1[pl.ds(z + 1, kz), pl.ds(y + 2, ky)] = (value - flux + x_prev(flux)) / (
            1.0 - cross + x_prev(cross)
        )

    def y_flux(z, y, kz, ky):
        rows = pl.ds(z, kz)
        face = (rows, pl.ds(y, ky))
        fy[face] = between(dt, refs1[3:], vy, face, face, (rows, pl.ds(y + 1, ky)))

    def y_update(z, y, kz, ky):
        rows = pl.ds(z, kz)
        low, high = pl.ds(y, ky), pl.ds(y + 1, ky)
        value = g1[pl.ds(z + 1, kz), pl.ds(y + 2, ky)]
        g2[pl.ds(z + 2, kz), pl.ds(y + 1, ky)] = (value - fy[rows, high] + fy[rows, low]) / (
            1.0 - dt * vy[rows, high] + dt * vy[rows, low]
        )

    middle_row = Z // 2 + 1
    halves = ((0, middle_row), (middle_row, Z))
    spans1 = []
    for depth in (1, 2):
        for low, high in halves:
            for dy in (-1, 1):
                src, dst = span(dy, Y, 2, 2)
                near = (0, 1)[(dy > 0) == (depth == 1)]
                rows = pl.ds(1 + low, high - low)
                spans1.append((
                    0, dy, rows, rows,
                    pl.ds(src.start + near, 1), pl.ds(dst.start + near, 1),
                ))
    deep = len(spans1)
    for dz in (-1, 1):
        spans1.append((dz, 0, *span(dz, Z, 1, 1), pl.ds(2, Y), pl.ds(2, Y)))
    spans1 += spans_for(CORNERS, 1, 2)
    halos1 = halo_copies(g1, spans1, halo1_send, halo1_recv)
    first = halos1[:deep // 2]
    second = halos1[deep // 2:deep]
    flat1, corners1 = halos1[deep:deep + 2], halos1[deep + 2:]

    for z in (0, Z - 1):
        for y in range(0, Y, Y // 2):
            x_update(z, y, 1, Y // 2)
    for copy in corners1 + flat1:
        copy.start()
    for copies, ys in ((first, (0, Y - 1)), (second, (1, Y - 2))):
        for at_half, (low, high) in enumerate(halves):
            both(x_update, range(max(low, 1), min(high, Z - 1)), ys)
            for copy in copies[2 * at_half:2 * at_half + 2]:
                copy.start()
    block(x_update, range(1, Z - 1), 2, Y - 4)
    smooth_own(refs1, 1, 2)
    block(planes(refs1, 1, 2), range(1, Z - 1), 2, Y - 2)
    for copy in flat1:
        copy.wait()
    ghost_rows(refs1, [(0, 2, 1, Y), (Z + 1, 2, 1, Y)])
    block(planes(refs1, 1, 2), (0, Z - 1), 2, Y - 2)
    block(y_flux, own, 2, 2)
    block(y_flux, own, 4, Y - 5)
    for copy in vel_copies:
        copy.wait()
    for at_half, (low, high) in enumerate(halves):
        for copy in first[2 * at_half:2 * at_half + 2]:
            copy.wait()
        ghost_rows(refs1, [(1 + low, y, high - low, 1) for y in (1, Y + 2)])
        both(planes(refs1, 1), range(max(low - 1, 1), high - 1), (1, Y), 1)

    per = Z // CHUNKS
    spans2 = []
    for low in range(0, Z, per):
        for dy in (-1, 1):
            rows = pl.ds(2 + low, per)
            spans2.append((0, dy, rows, rows, *span(dy, Y, 1, 1)))
    spans2 += spans_for(Z_SIDES + CORNERS, 2, 1)
    halos2 = halo_copies(g2, spans2, halo2_send, halo2_recv)
    side, flat, corners = halos2[:2 * CHUNKS], halos2[2 * CHUNKS:-4], halos2[-4:]

    def chunk_out(chunk):
        low, high = chunk * per, (chunk + 1) * per
        start, count = max(low, 1), min(high, Z - 1) - max(low, 1)
        for y in (0, Y + 1):
            plane(refs1, 1, start, y, count, 1)
        for y in (0, Y - 1):
            for z in range(low, high, 2):
                y_flux(z, y, 2, 2)
            y_update(low, y, per, 1)

    for at_half, (low, high) in enumerate(halves):
        for copy in second[2 * at_half:2 * at_half + 2] + corners1[2 - 2 * at_half:4 - 2 * at_half]:
            copy.wait()
        end = at_half * (Z - 1)
        ghost = at_half * (Z + 1)
        ghost_rows(refs1, [(1 + low, y, high - low, 1) for y in (0, Y + 3)])
        ghost_rows(refs1, [(ghost, 0, 1, 2), (ghost, Y + 2, 1, 2)])
        for y in (0, Y):
            plane(refs1, 1, end, y, 1, 2)
        chunk_out(at_half * (CHUNKS - 1))
        for z in (end, end + 1 - 2 * at_half):
            y_update(z, 1, 1, Y - 2)
        chunk = at_half * (CHUNKS - 1)
        for copy in (
            corners[2 * at_half:2 * at_half + 2] + [flat[at_half]]
            + side[2 * chunk:2 * chunk + 2]
        ):
            copy.start()
        chunk_out(1 + at_half)
        for copy in side[2 + 2 * at_half:4 + 2 * at_half]:
            copy.start()
    block(y_update, range(2, Z - 2), 1, Y - 2)

    smooth_own(refs2, 2, 1)
    block(planes(refs2, 0, 2), range(2, Z), 1, Y - 2)
    for copy in flat:
        copy.wait()
    ghost_rows(refs2, [(0, 1, 2, Y), (Z + 2, 1, 2, Y)])
    for zs in ((0, 1), (Z, Z + 1)):
        block(planes(refs2, 0, 2), zs, 1, Y - 2)

    def z_flux(z):
        for y in (1, Y // 2):
            face, above = (pl.ds(z, 1), pl.ds(y, 3)), (pl.ds(z + 1, 1), pl.ds(y, 3))
            fz[face] = between(dt, refs2[3:], vz, face, face, above)

    z_flux(0)
    loop(1, Z + 1, z_flux)

    def z_update(z):
        for y in range(1, Y - 1):
            value = (g2[z + 2, y + 1] - fz[z + 1, y] + fz[z, y]) / (
                1.0 - step_value * vz[z + 1, y] + step_value * vz[z, y]
            )
            middle[z, pl.ds(y, T, stride=Y), :] = value

    loop(0, Z, z_update)
    for copy in side[:4] + corners[2:]:
        copy.wait()
    first_rows = 2 + Z // 2
    ghost_rows(refs2, [(0, y, first_rows, 1) for y in (0, Y + 1)])
    both(planes(refs2, 0), range(0, first_rows - 2), (0, Y - 1))
    for y in (0, Y - 1):
        edge_flux(dt, refs2[3:], vz, fz, 0, per + 1, y, y)
        edge_update(g2, vz, fz, middle, step_value, range(0, per), Y, y, y)
    for copy in side[4:] + corners[:2]:
        copy.wait()
    ghost_rows(refs2, [(first_rows, y, Z + 4 - first_rows, 1) for y in (0, Y + 1)])
    both(planes(refs2, 0), range(first_rows - 2, Z + 2), (0, Y - 1))


def finish(
    middle, g2, vz, off, ta, tb, sd, step_ref, out_hbm, dt_hbm, fz, field, one, sems
):
    Z, T = middle.shape[0], step_ref.shape[0]
    Y = middle.shape[1] // T
    step = step_ref[...]
    one[...] = step[:1, :1]
    copies = [pltpu.make_async_copy(one, dt_hbm, sems.at[CHUNKS])]
    copies[0].start()
    dt = step[None, None]
    per = Z // CHUNKS
    for chunk in range(CHUNKS):
        low, high = chunk * per, (chunk + 1) * per
        if chunk > 0:
            for side, y in enumerate((0, Y - 1)):
                new = low if chunk == 1 else low + 1
                edge_flux(dt, (off, ta, tb, sd), vz, fz, new, high + 1, y, side)
                edge_update(g2, vz, fz, field, step, range(low, high), Y, y, side)
            for z in range(low, high):
                for y in range(1, Y - 1):
                    where = pl.ds(y, T, stride=Y)
                    field[z, where, :] = middle[z, where, :]
        part = pl.ds(low, per)
        source = field if chunk > 0 else middle
        copies.append(pltpu.make_async_copy(source.at[part], out_hbm.at[part], sems.at[chunk]))
        copies[-1].start()
    for copy in copies:
        copy.wait()


def solution(mesh):
    n_gy, n_gz = mesh.shape["gy"], mesh.shape["gz"]

    def shards(*blocks):
        Z, Y, X = blocks[0].shape
        T = X // LANES

        def split(block):
            return block.reshape(Z, Y, T, LANES).transpose(0, 2, 1, 3).reshape(Z, T * Y, LANES)

        def rows(*lead):
            return pltpu.VMEM((*lead, T, LANES), jnp.float32)

        dma = pltpu.SemaphoreType.DMA
        in_vmem = pl.BlockSpec(memory_space=pltpu.VMEM)
        kept = (
            pltpu.VMEM((Z, T * Y, LANES), jnp.float32),
            rows(Z + 4, Y + 2), rows(Z + 1, Y), *[rows(Z + 2, Y)] * 4,
        )
        state = pl.pallas_call(
            functools.partial(kernel, n_gy, n_gz),
            out_shape=(
                *kept, pltpu.VMEM((T, LANES), jnp.float32),
            ),
            in_specs=[pl.BlockSpec(memory_space=pltpu.HBM)] * 4,
            out_specs=(in_vmem,) * (len(kept) + 1),
            scratch_shapes=[
                *[pltpu.VMEM((Z, T * Y, LANES), jnp.float32)] * 4, dma((4,)),
                rows(Z + 2, Y + 2), rows(Z + 2, Y + 4),
                *[rows(Z + 2, Y + 2)] * 2, *[rows(Z + 2, Y + 4)] * 2, *[rows(Z + 4, Y + 2)] * 2,
                *[rows(Z, Y)] * 4, *[rows(Z, Y + 2)] * 4,
                rows(Z, Y), rows(Z, Y + 1), rows(Z, Y + 1), rows(Z + 1, Y),
                pltpu.VMEM((n_gy * n_gz, 1, LANES), jnp.float32),
                dma((8,)), dma((8,)), *[dma((4 * HALVES + 6,))] * 2, *[dma((2 * CHUNKS + 6,))] * 2,
                dma((2,)), dma((2,)),
                dma((2,)),
            ],
            compiler_params=pltpu.CompilerParams(
                collective_id=0, has_side_effects=True, vmem_limit_bytes=62640128
            ),
        )(*[split(block) for block in blocks])
        field, dt = pl.pallas_call(
            finish,
            out_shape=(
                jax.ShapeDtypeStruct((Z, T * Y, LANES), jnp.float32),
                jax.ShapeDtypeStruct((1, 1), jnp.float32),
            ),
            in_specs=[in_vmem] * len(state),
            out_specs=(pl.BlockSpec(memory_space=pltpu.HBM),) * 2,
            scratch_shapes=[
                rows(Z + 1, 2), pltpu.VMEM((Z, T * Y, LANES), jnp.float32),
                pltpu.VMEM((1, 1), jnp.float32), dma((CHUNKS + 1,)),
            ],
            compiler_params=pltpu.CompilerParams(vmem_limit_bytes=16777216),
        )(
            *[pltpu.with_memory_space_constraint(value, pltpu.VMEM) for value in state],
        )
        field = field.reshape(Z, T, Y, LANES).transpose(0, 2, 1, 3).reshape(Z, Y, X)
        return field, dt.reshape(())

    spec = P("gz", "gy", None)
    return jax.shard_map(
        shards, mesh=mesh, in_specs=(spec,) * 4, out_specs=(spec, P()), check_vma=False
    )
```

```python
import functools

import jax
import jax.numpy as jnp
from jax import lax
from jax.experimental import pallas as pl
from jax.experimental.pallas import tpu as pltpu
from jax.sharding import PartitionSpec as P

NEWTON = 5
CHUNKS = 4
HALVES = 2
LANES = 128
GROUP = 8

tilt_floor = 3.2
courant = 0.45
epsilon = 1e-06
tiny = 1e-30
tiny_unit = 1e-15

MESH = pl.DeviceIdType.MESH


def lane_of(value):
    return lax.broadcasted_iota(jnp.int32, value.shape, value.ndim - 1)


def x_next(value):
    turned = pltpu.roll(value, LANES - 1, value.ndim - 1)
    carried = pltpu.roll(turned, value.shape[-2] - 1, value.ndim - 2)
    return jnp.where(lane_of(value) == LANES - 1, carried, turned)


def x_prev(value):
    turned = pltpu.roll(value, 1, value.ndim - 1)
    carried = pltpu.roll(turned, 1, value.ndim - 2)
    return jnp.where(lane_of(value) == 0, carried, turned)


def solve_offset(g, tilt_a, tilt_b, tilt_d):
    volume = jnp.clip(g, 0.0, 1.0)
    lesser = jnp.minimum(volume, 1.0 - volume)
    low = jnp.minimum(tilt_a, tilt_b)
    high = jnp.maximum(tilt_a, tilt_b)
    unit = jnp.maximum(jnp.minimum(low, tilt_d), tiny_unit)
    middle = jnp.maximum(low, tilt_d)
    inverse = 1.0 / unit
    n2 = jnp.minimum(middle, high) * inverse
    n3 = jnp.maximum(middle, high) * inverse
    above = n2 + 1.0
    summed = above + n3
    product = n2 * n3
    target = product * (lesser + lesser)
    gap = 0.5 * jnp.maximum(above - n3, 0.0)
    offset = 0.5 * (summed - (product - target) / (n2 - gap * gap))
    for repeat in range(NEWTON - 1):
        p1 = jnp.minimum(offset, 1.0)
        p2 = jnp.clip(offset - n2, 0.0, 1.0)
        p3 = jnp.maximum(offset - n3, 0.0)
        s1, s2, s3 = p1 * p1, p2 * p2, p3 * p3
        squares = s1 - s2 - s3
        cubes = s1 * p1 - s2 * p2 - s3 * p3
        outer = jnp.clip(offset, 1.0, above)
        q = outer - 1.0
        rate = squares + (q + q)
        offset = (offset * squares - cubes * (1.0 / 3.0) + (q * outer + target)) / rate
    return jnp.where(volume > 0.5, summed - offset, offset) * unit


def face_flux(cross, offset, tilt_a, tilt_b, slope):
    turn = slope * cross
    height = jnp.abs(turn)
    reach = offset - jnp.where(turn > 0, 0.0, jnp.abs(slope) - height)

    def parts(value):
        inside = jnp.maximum(value, 0.0)
        p = jnp.minimum(inside, height)
        q = inside - p
        return p * p * p, q * (q + height)

    reach_a = reach - tilt_a
    p0, q0 = parts(reach)
    p1, q1 = parts(reach_a)
    p2, q2 = parts(reach - tilt_b)
    p3, q3 = parts(reach_a - tilt_b)
    cubes = (p0 - p1) - (p2 - p3)
    wholes = (q0 - q1) - (q2 - q3)
    combo = cubes * ((1.0 / 3.0) / jnp.maximum(height, tiny)) + wholes
    return cross * combo / (2.0 * tilt_a * tilt_b)


def between(dt, planes, velocity, at_face, below, above):
    cross = dt * velocity[at_face]
    upward = cross > 0
    donor = [jnp.where(upward, ref[below], ref[above]) for ref in planes]
    return face_flux(cross, *donor)


def edge_flux(dt, planes, velocity, flux, low, high, y, column):
    while low < high:
        count = min(2, high - low)
        face, above = (pl.ds(low, count), pl.ds(y, 1)), (pl.ds(low + 1, count), pl.ds(y, 1))
        flux[pl.ds(low, count), pl.ds(column, 1)] = between(dt, planes, velocity, face, face, above)
        low += count


def edge_update(g, velocity, flux, field, step, planes, Y, y, column):
    for z in planes:
        value = (g[z + 2, y + 1] - flux[z + 1, column] + flux[z, column]) / (
            1.0 - step * velocity[z + 1, y] + step * velocity[z, y]
        )
        field[z, pl.ds(y, value.shape[0], stride=Y), :] = value


def kernel(
    n_gy, n_gz, f_hbm, vx_hbm, vy_hbm, vz_hbm,
    middle, g2, vz, off2, ta2, tb2, sd2, step_ref,
    f_ref, vx_ref, vy_ref, vz_ref, load_sem,
    g0, g1, sx0, dx0, sx1, dx1, sx2, dx2,
    off0, ta0, tb0, sd0, off1, ta1, tb1, sd1,
    vx, vy, fy, fz, part,
    halo0_send, halo0_recv, halo1_send, halo1_recv, halo2_send, halo2_recv,
    vel_send, vel_recv, part_sem,
):
    Z = f_ref.shape[0]
    T = sx0.shape[2]
    Y = f_ref.shape[1] // T
    loads = []
    for i, (source, target) in enumerate(
        ((f_hbm, f_ref), (vx_hbm, vx_ref), (vy_hbm, vy_ref), (vz_hbm, vz_ref))
    ):
        loads.append(pltpu.make_async_copy(source, target, load_sem.at[i]))
        loads[-1].start()
    my = lax.axis_index("gy")
    mz = lax.axis_index("gz")

    def at(dz, dy):
        return {
            "gy": lax.rem(my + dy + n_gy, n_gy),
            "gz": lax.rem(mz + dz + n_gz, n_gz),
        }

    barrier = pltpu.get_barrier_semaphore()
    def hops(away):
        steps = (away[0] // 2, away[1] // 4, away[1] % 4)
        return sum(min(step, 4 - step) for step in steps)

    greeted = [(a, b) for a in range(n_gz) for b in range(n_gy)][1:]
    greeted.sort(key=hops, reverse=True)
    far = sum(hops(away) >= 5 for away in greeted)
    for dz, dy in greeted:
        pl.semaphore_signal(barrier, inc=1, device_id=at(dz, dy), device_id_type=MESH)

    def rows_of(ref, z, y):
        return ref[z, pl.ds(y, T, stride=Y), :]

    def gather(low, high, body, carry, most=GROUP):
        count = high - low
        grouped = max(u for u in range(1, most + 1) if count % u == 0)

        def step(i, carry):
            for u in range(grouped):
                carry = body(low + i * grouped + u, carry)
            return carry
        return lax.fori_loop(0, count // grouped, step, carry)

    def loop(low, high, body, most=GROUP):
        def step(i, carry):
            body(i)
            return carry
        gather(low, high, step, 0, most)

    def halo_copies(g, spans, sends, recvs):
        copies = []
        for index, (dz, dy, src_z, dst_z, src_y, dst_y) in enumerate(spans):
            copies.append(pltpu.make_async_remote_copy(
                src_ref=g.at[src_z, src_y],
                dst_ref=g.at[dst_z, dst_y],
                send_sem=sends.at[index],
                recv_sem=recvs.at[index],
                device_id=at(dz, dy),
                device_id_type=MESH,
            ))
        return copies

    def span(side, count, pad, depth):
        if side == 0:
            return pl.ds(pad, count), pl.ds(pad, count)
        if side > 0:
            return pl.ds(pad + count - depth, depth), pl.ds(pad - depth, depth)
        return pl.ds(pad, depth), pl.ds(pad + count, depth)

    def spans_for(sides, pad_z, pad_y):
        return [
            (dz, dy, *span(dz, Z, pad_z, pad_z), *span(dy, Y, pad_y, pad_y))
            for dz, dy in sides
        ]

    Y_SIDES = [(0, -1), (0, 1)]
    Z_SIDES = [(-1, 0), (1, 0)]
    CORNERS = [(a, b) for a in (-1, 1) for b in (-1, 1)]

    def smooth_rows(g, sx, dx, z, y, kz, ky):
        value = g[pl.ds(z, kz), pl.ds(y, ky)]
        after, before = x_next(value), x_prev(value)
        sx[pl.ds(z, kz), pl.ds(y, ky)] = before + (value + value) + after
        dx[pl.ds(z, kz), pl.ds(y, ky)] = after - before

    def smooth_zero(arr):
        mid = arr[1:-1]
        return (arr[:-2] + mid) + (mid + arr[2:])

    def smooth_one(arr):
        pair = arr[:, :-1] + arr[:, 1:]
        return pair[:, :-1] + pair[:, 1:]

    def plane(refs, dim, z, y, kz, ky, parts=1):
        g, sx, dx, off, ta, tb, sd = refs
        s = sx[pl.ds(z, kz + 2), pl.ds(y, ky + 2)]
        d = dx[pl.ds(z, kz + 2), pl.ds(y, ky + 2)]
        grad_zero = smooth_one(s[2:] - s[:-2])
        across = smooth_zero(s)
        grad_one = (across[:, 2:] - across[:, :-2])
        grad_cells = smooth_one(smooth_zero(d))
        slopes = (grad_zero, grad_one, grad_cells)
        low = 0
        for part in range(parts):
            count = (ky - low) // (parts - part)
            cut = [value[:, low:low + count] for value in slopes]
            slope = cut[dim]
            tilt_a, tilt_b = [jnp.abs(cut[e]) + tilt_floor for e in range(3) if e != dim]
            value = g[pl.ds(z + 1, kz), pl.ds(y + 1 + low, count)]
            where = (pl.ds(z, kz), pl.ds(y + low, count))
            off[where] = solve_offset(value, tilt_a, tilt_b, jnp.abs(slope))
            ta[where] = tilt_a
            tb[where] = tilt_b
            sd[where] = slope
            low += count

    def block(body, zs, y, ky, kz=1):
        count = len(zs) // kz
        step = zs[1] - zs[0] if len(zs) > 1 else 1
        loop(0, count, lambda i: body(zs[0] + step * kz * i, y, kz, ky))

    def both(body, zs, ys, kz=2):
        count = len(zs) // kz

        def step(i):
            for y in ys:
                body(zs[0] + kz * i, y, kz, 1)
        loop(0, count, step)

    def planes(refs, dim, parts=1):
        return lambda z, y, kz, ky: plane(refs, dim, z, y, kz, ky, parts)

    def smooth_own(refs, z, y):
        loop(z, z + Z, lambda i: smooth_rows(*refs[:3], i, y, 1, Y), Z)

    own = range(0, Z)
    refs0 = (g0, sx0, dx0, off0, ta0, tb0, sd0)
    refs1 = (g1, sx1, dx1, off1, ta1, tb1, sd1)
    refs2 = (g2, sx2, dx2, off2, ta2, tb2, sd2)

    def donors(z, y, kz, ky):
        where = (pl.ds(z, kz), pl.ds(y, ky))
        upward = vx[where] > 0
        for ref in (off0, ta0, tb0, sd0):
            value = ref[where]
            ref[where] = jnp.where(upward, value, x_next(value))

    def donors_in():
        loop(1, Z - 1, lambda z: donors(z, 1, 1, Y - 2))

    def ghost_rows(refs, spans):
        for z, y, kz, ky in spans:
            smooth_rows(*refs[:3], z, y, kz, ky)

    def fill(z, total):
        for y in range(Y):
            f = rows_of(f_ref, z, y)
            g0[z + 1, y + 1] = f
            total = total + 4.0 * f * (1.0 - f)
        return total

    loads[0].wait()
    total = gather(0, Z, fill, jnp.zeros((T, LANES), jnp.float32))

    def fill_velocity(z, peak):
        for y in range(Y):
            a = rows_of(vx_ref, z, y)
            b = rows_of(vy_ref, z, y)
            c = rows_of(vz_ref, z, y)
            vx[z, y] = a
            vy[z, y + 1] = b
            vz[z + 1, y] = c
            peak = jnp.maximum(peak, jnp.maximum(jnp.abs(a), jnp.maximum(jnp.abs(b), jnp.abs(c))))
        return peak

    for copy in loads[1:]:
        copy.wait()
    peak = gather(0, Z, fill_velocity, jnp.zeros((T, LANES), jnp.float32))
    low_lanes = lane_of(jnp.zeros((1, LANES), jnp.float32)) < LANES // 2

    def folded(sums, peaks):
        sums = jnp.sum(sums, axis=0, keepdims=True)
        peaks = jnp.max(peaks, axis=0, keepdims=True)
        sums = sums + pltpu.roll(sums, LANES // 2, 1)
        peaks = jnp.maximum(peaks, pltpu.roll(peaks, LANES // 2, 1))
        return jnp.where(low_lanes, sums, peaks)

    me = mz * n_gy + my
    part[me] = folded(total, peak)
    pl.semaphore_wait(barrier, len(greeted))
    vel_copies = [
        pltpu.make_async_remote_copy(
            src_ref=vy.at[:, pl.ds(Y, 1)], dst_ref=vy.at[:, pl.ds(0, 1)],
            send_sem=vel_send.at[0], recv_sem=vel_recv.at[0],
            device_id=at(0, 1), device_id_type=MESH,
        ),
        pltpu.make_async_remote_copy(
            src_ref=vz.at[pl.ds(Z, 1)], dst_ref=vz.at[pl.ds(0, 1)],
            send_sem=vel_send.at[1], recv_sem=vel_recv.at[1],
            device_id=at(1, 0), device_id_type=MESH,
        ),
    ]

    halos0 = halo_copies(
        g0, spans_for(Y_SIDES + Z_SIDES + CORNERS, 1, 1), halo0_send, halo0_recv
    )
    part_copies = [
        pltpu.make_async_remote_copy(
            src_ref=part.at[me], dst_ref=part.at[me],
            send_sem=part_sem.at[0], recv_sem=part_sem.at[1],
            device_id=at(*away), device_id_type=MESH,
        )
        for away in greeted
    ]
    for copy in halos0[4:] + halos0[2:4] + part_copies[:far] + halos0[:2] + part_copies[far:]:
        copy.start()

    smooth_own(refs0, 1, 1)
    block(planes(refs0, 2, 2), range(1, Z - 1), 1, Y - 2)
    donors_in()
    for copy in vel_copies:
        copy.start()
    for copy in halos0[2:4]:
        copy.wait()
    ghost_rows(refs0, [(0, 1, 1, Y), (Z + 1, 1, 1, Y)])
    block(planes(refs0, 2, 2), (0, Z - 1), 1, Y - 2)
    for z in (0, Z - 1):
        donors(z, 1, 1, Y - 2)
    for copy in halos0[:2] + halos0[4:]:
        copy.wait()
    ghost_rows(refs0, [(0, 0, Z + 2, 1), (0, Y + 1, Z + 2, 1)])
    both(planes(refs0, 2), own, (0, Y - 1))
    both(donors, own, (0, Y - 1), 4)
    others = pl.ds(0, len(greeted))
    arrived = pltpu.make_async_remote_copy(
        src_ref=part.at[others], dst_ref=part.at[others],
        send_sem=part_sem.at[0], recv_sem=part_sem.at[1],
        device_id=at(*greeted[0]), device_id_type=MESH,
    )
    arrived.wait()
    sums = [part[i] for i in range(GROUP)]
    peaks = list(sums)
    for i in range(len(sums), n_gy * n_gz):
        at_row = i % len(sums)
        row = part[i]
        sums[at_row] = sums[at_row] + row
        peaks[at_row] = jnp.maximum(peaks[at_row], row)
    while len(sums) > 1:
        count = len(sums) // 2
        sums = [sums[i] + sums[i + count] for i in range(count)]
        peaks = [jnp.maximum(peaks[i], peaks[i + count]) for i in range(count)]
    sums, peaks = sums[0], peaks[0]
    sums = jnp.where(low_lanes, sums, 0.0)
    peaks = jnp.where(low_lanes, 0.0, peaks)
    cells_all = float(Z * Y * T * LANES * n_gy * n_gz)
    share = jnp.broadcast_to(jnp.sum(sums, keepdims=True), (T, LANES)) / cells_all
    umax = jnp.broadcast_to(jnp.max(peaks, keepdims=True), (T, LANES))
    step_value = courant / ((umax + epsilon) * (1.0 + share))
    step_ref[...] = step_value
    dt = step_value[None, None]

    def x_update(z, y, kz, ky):
        where = (pl.ds(z, kz), pl.ds(y, ky))
        cross = dt * vx[where]
        flux = face_flux(cross, off0[where], ta0[where], tb0[where], sd0[where])
        value = g0[pl.ds(z + 1, kz), pl.ds(y + 1, ky)]
        g1[pl.ds(z + 1, kz), pl.ds(y + 2, ky)] = (value - flux + x_prev(flux)) / (
            1.0 - cross + x_prev(cross)
        )

    def y_flux(z, y, kz, ky):
        rows = pl.ds(z, kz)
        face = (rows, pl.ds(y, ky))
        fy[face] = between(dt, refs1[3:], vy, face, face, (rows, pl.ds(y + 1, ky)))

    def y_update(z, y, kz, ky):
        rows = pl.ds(z, kz)
        low, high = pl.ds(y, ky), pl.ds(y + 1, ky)
        value = g1[pl.ds(z + 1, kz), pl.ds(y + 2, ky)]
        g2[pl.ds(z + 2, kz), pl.ds(y + 1, ky)] = (value - fy[rows, high] + fy[rows, low]) / (
            1.0 - dt * vy[rows, high] + dt * vy[rows, low]
        )

    middle_row = Z // 2 + 1
    halves = ((0, middle_row), (middle_row, Z))
    spans1 = []
    for depth in (1, 2):
        for low, high in halves:
            for dy in (-1, 1):
                src, dst = span(dy, Y, 2, 2)
                near = (0, 1)[(dy > 0) == (depth == 1)]
                rows = pl.ds(1 + low, high - low)
                spans1.append((
                    0, dy, rows, rows,
                    pl.ds(src.start + near, 1), pl.ds(dst.start + near, 1),
                ))
    deep = len(spans1)
    for dz in (-1, 1):
        spans1.append((dz, 0, *span(dz, Z, 1, 1), pl.ds(2, Y), pl.ds(2, Y)))
    spans1 += spans_for(CORNERS, 1, 2)
    halos1 = halo_copies(g1, spans1, halo1_send, halo1_recv)
    first = halos1[:deep // 2]
    second = halos1[deep // 2:deep]
    flat1, corners1 = halos1[deep:deep + 2], halos1[deep + 2:]

    for z in (0, Z - 1):
        for y in range(0, Y, Y // 2):
            x_update(z, y, 1, Y // 2)
    for copy in corners1 + flat1:
        copy.start()
    for copies, ys in ((first, (0, Y - 1)), (second, (1, Y - 2))):
        for at_half, (low, high) in enumerate(halves):
            both(x_update, range(max(low, 1), min(high, Z - 1)), ys)
            for copy in copies[2 * at_half:2 * at_half + 2]:
                copy.start()
    block(x_update, range(1, Z - 1), 2, Y - 4)
    smooth_own(refs1, 1, 2)
    block(planes(refs1, 1, 2), range(1, Z - 1), 2, Y - 2)
    for copy in flat1:
        copy.wait()
    ghost_rows(refs1, [(0, 2, 1, Y), (Z + 1, 2, 1, Y)])
    block(planes(refs1, 1, 2), (0, Z - 1), 2, Y - 2)
    block(y_flux, own, 2, 2)
    block(y_flux, own, 4, Y - 5)
    for copy in vel_copies:
        copy.wait()
    for at_half, (low, high) in enumerate(halves):
        for copy in first[2 * at_half:2 * at_half + 2]:
            copy.wait()
        ghost_rows(refs1, [(1 + low, y, high - low, 1) for y in (1, Y + 2)])
        both(planes(refs1, 1), range(max(low - 1, 1), high - 1), (1, Y), 1)

    per = Z // CHUNKS
    spans2 = []
    for low in range(0, Z, per):
        for dy in (-1, 1):
            rows = pl.ds(2 + low, per)
            spans2.append((0, dy, rows, rows, *span(dy, Y, 1, 1)))
    spans2 += spans_for(Z_SIDES + CORNERS, 2, 1)
    halos2 = halo_copies(g2, spans2, halo2_send, halo2_recv)
    side, flat, corners = halos2[:2 * CHUNKS], halos2[2 * CHUNKS:-4], halos2[-4:]

    def chunk_out(chunk):
        low, high = chunk * per, (chunk + 1) * per
        start, count = max(low, 1), min(high, Z - 1) - max(low, 1)
        for y in (0, Y + 1):
            plane(refs1, 1, start, y, count, 1)
        for y in (0, Y - 1):
            for z in range(low, high, 2):
                y_flux(z, y, 2, 2)
            y_update(low, y, per, 1)

    for at_half, (low, high) in enumerate(halves):
        for copy in second[2 * at_half:2 * at_half + 2] + corners1[2 - 2 * at_half:4 - 2 * at_half]:
            copy.wait()
        end = at_half * (Z - 1)
        ghost = at_half * (Z + 1)
        ghost_rows(refs1, [(1 + low, y, high - low, 1) for y in (0, Y + 3)])
        ghost_rows(refs1, [(ghost, 0, 1, 2), (ghost, Y + 2, 1, 2)])
        for y in (0, Y):
            plane(refs1, 1, end, y, 1, 2)
        chunk_out(at_half * (CHUNKS - 1))
        for z in (end, end + 1 - 2 * at_half):
            y_update(z, 1, 1, Y - 2)
        chunk = at_half * (CHUNKS - 1)
        for copy in (
            corners[2 * at_half:2 * at_half + 2] + [flat[at_half]]
            + side[2 * chunk:2 * chunk + 2]
        ):
            copy.start()
        chunk_out(1 + at_half)
        for copy in side[2 + 2 * at_half:4 + 2 * at_half]:
            copy.start()
    block(y_update, range(2, Z - 2), 1, Y - 2)

    smooth_own(refs2, 2, 1)
    block(planes(refs2, 0, 2), range(2, Z), 1, Y - 2)
    for copy in flat:
        copy.wait()
    ghost_rows(refs2, [(0, 1, 2, Y), (Z + 2, 1, 2, Y)])
    for zs in ((0, 1), (Z, Z + 1)):
        block(planes(refs2, 0, 2), zs, 1, Y - 2)

    def z_flux(z):
        for y in (1, Y // 2):
            face, above = (pl.ds(z, 1), pl.ds(y, 3)), (pl.ds(z + 1, 1), pl.ds(y, 3))
            fz[face] = between(dt, refs2[3:], vz, face, face, above)

    z_flux(0)
    loop(1, Z + 1, z_flux)

    def z_update(z):
        for y in range(1, Y - 1):
            value = (g2[z + 2, y + 1] - fz[z + 1, y] + fz[z, y]) / (
                1.0 - step_value * vz[z + 1, y] + step_value * vz[z, y]
            )
            middle[z, pl.ds(y, T, stride=Y), :] = value

    loop(0, Z, z_update)
    for copy in side[:4] + corners[2:]:
        copy.wait()
    first_rows = 2 + Z // 2
    ghost_rows(refs2, [(0, y, first_rows, 1) for y in (0, Y + 1)])
    both(planes(refs2, 0), range(0, first_rows - 2), (0, Y - 1))
    for y in (0, Y - 1):
        edge_flux(dt, refs2[3:], vz, fz, 0, per + 1, y, y)
        edge_update(g2, vz, fz, middle, step_value, range(0, per), Y, y, y)
    for copy in side[4:] + corners[:2]:
        copy.wait()
    ghost_rows(refs2, [(first_rows, y, Z + 4 - first_rows, 1) for y in (0, Y + 1)])
    both(planes(refs2, 0), range(first_rows - 2, Z + 2), (0, Y - 1))


def finish(
    middle, g2, vz, off, ta, tb, sd, step_ref, out_hbm, dt_hbm, fz, field, one, sems
):
    Z, T = middle.shape[0], step_ref.shape[0]
    Y = middle.shape[1] // T
    step = step_ref[...]
    one[...] = step[:1, :1]
    copies = [pltpu.make_async_copy(one, dt_hbm, sems.at[CHUNKS])]
    copies[0].start()
    dt = step[None, None]
    per = Z // CHUNKS
    for chunk in range(CHUNKS):
        low, high = chunk * per, (chunk + 1) * per
        if chunk > 0:
            for side, y in enumerate((0, Y - 1)):
                new = low if chunk == 1 else low + 1
                edge_flux(dt, (off, ta, tb, sd), vz, fz, new, high + 1, y, side)
                edge_update(g2, vz, fz, field, step, range(low, high), Y, y, side)
            for z in range(low, high):
                for y in range(1, Y - 1):
                    where = pl.ds(y, T, stride=Y)
                    field[z, where, :] = middle[z, where, :]
        part = pl.ds(low, per)
        source = field if chunk > 0 else middle
        copies.append(pltpu.make_async_copy(source.at[part], out_hbm.at[part], sems.at[chunk]))
        copies[-1].start()
    for copy in copies:
        copy.wait()


def solution(mesh):
    n_gy, n_gz = mesh.shape["gy"], mesh.shape["gz"]

    def shards(*blocks):
        Z, Y, X = blocks[0].shape
        T = X // LANES

        def split(block):
            return block.reshape(Z, Y, T, LANES).transpose(0, 2, 1, 3).reshape(Z, T * Y, LANES)

        def rows(*lead):
            return pltpu.VMEM((*lead, T, LANES), jnp.float32)

        dma = pltpu.SemaphoreType.DMA
        in_vmem = pl.BlockSpec(memory_space=pltpu.VMEM)
        kept = (
            pltpu.VMEM((Z, T * Y, LANES), jnp.float32),
            rows(Z + 4, Y + 2), rows(Z + 1, Y), *[rows(Z + 2, Y)] * 4,
        )
        state = pl.pallas_call(
            functools.partial(kernel, n_gy, n_gz),
            out_shape=(
                *kept, pltpu.VMEM((T, LANES), jnp.float32),
            ),
            in_specs=[pl.BlockSpec(memory_space=pltpu.HBM)] * 4,
            out_specs=(in_vmem,) * (len(kept) + 1),
            scratch_shapes=[
                *[pltpu.VMEM((Z, T * Y, LANES), jnp.float32)] * 4, dma((4,)),
                rows(Z + 2, Y + 2), rows(Z + 2, Y + 4),
                *[rows(Z + 2, Y + 2)] * 2, *[rows(Z + 2, Y + 4)] * 2, *[rows(Z + 4, Y + 2)] * 2,
                *[rows(Z, Y)] * 4, *[rows(Z, Y + 2)] * 4,
                rows(Z, Y), rows(Z, Y + 1), rows(Z, Y + 1), rows(Z + 1, Y),
                pltpu.VMEM((n_gy * n_gz, 1, LANES), jnp.float32),
                dma((8,)), dma((8,)), *[dma((4 * HALVES + 6,))] * 2, *[dma((2 * CHUNKS + 6,))] * 2,
                dma((2,)), dma((2,)),
                dma((2,)),
            ],
            compiler_params=pltpu.CompilerParams(
                collective_id=0, has_side_effects=True, vmem_limit_bytes=62640128
            ),
        )(*[split(block) for block in blocks])
        field, dt = pl.pallas_call(
            finish,
            out_shape=(
                jax.ShapeDtypeStruct((Z, T * Y, LANES), jnp.float32),
                jax.ShapeDtypeStruct((1, 1), jnp.float32),
            ),
            in_specs=[in_vmem] * len(state),
            out_specs=(pl.BlockSpec(memory_space=pltpu.HBM),) * 2,
            scratch_shapes=[
                rows(Z + 1, 2), pltpu.VMEM((Z, T * Y, LANES), jnp.float32),
                pltpu.VMEM((1, 1), jnp.float32), dma((CHUNKS + 1,)),
            ],
            compiler_params=pltpu.CompilerParams(vmem_limit_bytes=16777216),
        )(
            *[pltpu.with_memory_space_constraint(value, pltpu.VMEM) for value in state],
        )
        field = field.reshape(Z, T, Y, LANES).transpose(0, 2, 1, 3).reshape(Z, Y, X)
        return field, dt.reshape(())

    spec = P("gz", "gy", None)
    return jax.shard_map(
        shards, mesh=mesh, in_specs=(spec,) * 4, out_specs=(spec, P()), check_vma=False
    )
```
